1024 devices in a mesh: sfc: 128 (over z, y), sub: 8 (over x, core).
Axes of the slice: x: 4, y: 8, z: 16, core: 2. Of those that a mesh axis runs over, the one named last changes fastest.
Arguments:
- vectors: float32 [64, 16384, 256], P(None, ('sfc', 'sub')), may hold values from -10 to 10
- reaction: float32 [16384, 256], P(('sfc', 'sub')), may hold values from 0.5 to 5
Outputs:
- basis: float32 [64, 16384, 256], P(None, ('sfc', 'sub'))
- upper: float32 [64, 64], replicated
The draws below stay inside these ranges and needn't reach their ends.
All inputs are finite; a program needn't handle non-finite values.
Results may differ from the reference program's by a relative error of at most 0.0003.
Values sent between devices are 32-bit elements; how exact they have to be, the bound alone decides.
No kernel may reach another device: no remote copies, remote signals or barrier semaphores. Data moves between devices by JAX's collectives and lax.ppermute only.
A program may use at most 32 MiB of HBM per device.

```python
import math
import jax
import jax.numpy as jnp
from jax import lax

K = 64
NY = 32
NL = 8
POWERS = 3
PLANE = 256
NX = 16384


def draw_vectors(key, part):
    key_shared, key_mixing, key_separate, key_ranking = jax.random.split(jax.random.fold_in(key, 71), 4)
    shared_count = 4
    smallest = 0.01
    shared = jax.random.normal(key_shared, (shared_count, NX, PLANE), jnp.float32)
    separate = jax.random.normal(key_separate, (K, NX, PLANE), jnp.float32)
    mixing = jax.random.normal(key_mixing, (shared_count, K), jnp.float32)
    ranking = jax.random.permutation(key_ranking, K).astype(jnp.float32)
    column_scale = jnp.power(jnp.float32(smallest), ranking / (K - 1))
    common = jnp.einsum('rk,rxp->kxp', mixing, shared) / math.sqrt(shared_count)
    combined = common + column_scale[:, None, None] * separate
    return jnp.clip(combined, -10.0, 10.0).astype(jnp.float32)


def block_scale(own_key, dims, pieces, least, top_value):
    level = 1.0
    for dim, blocks in pieces:
        steps = jax.random.uniform(jax.random.fold_in(jax.random.fold_in(own_key, 6), dim), (blocks,), jnp.float32, least / len(pieces), top_value / len(pieces))
        level = level * jnp.repeat(jnp.exp(steps), dims[dim] // blocks).reshape((-1,) + (1,) * (len(dims) - 1 - dim))
    return level


def setup_inputs(seed: int = 0) -> dict:
    arg_keys = jax.random.split(jax.random.key(seed), 3)
    return {
        "vectors": draw_vectors(jax.random.fold_in(arg_keys[2], 71), 0),
        "reaction": jnp.clip(jnp.exp(math.log(5.0) - 2.3025851 * jax.random.uniform(arg_keys[1], (NX, PLANE), jnp.float32) ** block_scale(arg_keys[1], (NX, PLANE), ((0, 1024),), -0.2, 0.2)), 0.5, 5.0),
    }


DELTA_MASS = 0.5

def line_tables(count):
    index = jnp.arange(count)
    offset = index[:, None] - index[None, :]
    near = (jnp.abs(offset) == 1).astype(jnp.float32)
    same = (offset == 0).astype(jnp.float32)
    mass = (4.0 * same + near) / 6.0
    stiff = 2.0 * same - near
    return (mass, stiff)

def tables(across, layers):
    mass_across, stiff_across = line_tables(across)
    mass_layers, stiff_layers = line_tables(layers)
    mass_plane = jnp.kron(mass_layers, mass_across)
    stiff_plane = jnp.kron(mass_layers, stiff_across) + jnp.kron(stiff_layers, mass_across) + DELTA_MASS * mass_plane
    return jnp.concatenate([mass_plane, stiff_plane], axis=1)

def operate(field, reaction, table):
    plane = table.shape[0]
    both = jnp.einsum('kzp,pq->kzq', field, table, precision=lax.Precision.HIGHEST)
    massed = both[..., :plane]
    mixed = both[..., plane:]
    edge_term = mixed / 6.0 - massed
    padded = jnp.pad(edge_term, ((0, 0), (1, 1), (0, 0)))
    return padded[:, :-2] + padded[:, 2:] + 4.0 / 6.0 * mixed + 2.0 * massed + reaction[None] * field

def lower_solve(lower, block):
    return lax.linalg.triangular_solve(lower, block, left_side=True, lower=True)

def reference(vectors, reaction):
    table = tables(NY, NL)
    groups = vectors.reshape(K // 8, 8, NX, NY * NL)

    def power(group):
        field = group
        for _ in range(POWERS):
            field = operate(field, reaction, table)
        return field
    applied = lax.map(power, groups).reshape(K, NX * NY * NL)
    gram = jnp.dot(applied, applied.T, precision=lax.Precision.HIGHEST)
    lower_one = jnp.linalg.cholesky(gram)
    first = lower_solve(lower_one, applied)
    gram_two = jnp.dot(first, first.T, precision=lax.Precision.HIGHEST)
    lower_two = jnp.linalg.cholesky(gram_two)
    second = lower_solve(lower_two, first)
    scale = math.sqrt(NX * NY * NL)
    upper = jnp.dot(lower_one, lower_two, precision=lax.Precision.HIGHEST).T / scale
    return ((second * scale).reshape(K, NX, NY * NL), upper)
```

```python
import math

import jax
import jax.numpy as jnp
from jax import lax
from jax.experimental import pallas as pl
from jax.experimental.pallas import tpu as pltpu
from jax.sharding import Mesh
from jax.sharding import PartitionSpec as P

NY = 32
NL = 8
PLANE = NY * NL
POWERS = 3
SFC_SUB = ("sfc_0", "sfc_1", "sub_0", "sub_1")
FAR = ("sfc_0",)
NEAR = ("sfc_1", "sub_0", "sub_1")
DELTA_MASS = 0.5
F32 = jnp.float32
BF16 = jnp.bfloat16
HIGHEST = lax.Precision.HIGHEST


def line_tables(count):
    index = jnp.arange(count)
    offset = index[:, None] - index[None, :]
    near = (jnp.abs(offset) == 1).astype(F32)
    same = (offset == 0).astype(F32)
    return 4.0 * same + near, 2.0 * same - near


def tables():
    mass_across, stiff_across = line_tables(NY)
    mass_layers, stiff_layers = line_tables(NL)
    mass = jnp.kron(mass_layers, mass_across)
    stiff = (
        6.0 * (jnp.kron(mass_layers, stiff_across) + jnp.kron(stiff_layers, mass_across))
        + DELTA_MASS * mass
    )
    return jnp.concatenate([stiff - 6.0 * mass, 4.0 * stiff + 12.0 * mass], axis=1).astype(BF16)


def split3(value):
    one = value.astype(BF16)
    rest = value - one.astype(F32)
    two = rest.astype(BF16)
    three = (rest - two.astype(F32)).astype(BF16)
    return one, two, three


def dot(a, b):
    return lax.dot_general(a, b, (((1,), (0,)), ((), ())), preferred_element_type=F32)


def dot_t(a, b):
    return lax.dot_general(a, b, (((1,), (1,)), ((), ())), preferred_element_type=F32)


def two_sum(a, b):
    s = a + b
    t = s - a
    return s, (a - (s - t)) + (b - t)


def power_below(x, square=False):
    low = -60 if square else -120
    p = jnp.full_like(x, 2.0**low)
    q = jnp.full_like(x, 2.0**-low)
    for k in (64, 32, 16, 8, 4, 2, 1) if square else (128, 64, 32, 16, 8, 4, 2, 1):
        half = 2.0 ** (k // 2) if k > 1 else 2.0
        up = p * half * (half if k > 1 else 1.0)
        down = q * (1.0 / half) * (1.0 / half if k > 1 else 1.0)
        fits = (up * up if square else up) <= x
        p, q = jnp.where(fits, up, p), jnp.where(fits, down, q)
    return p, q


def digits(value, count, extra=None, extra_at=3):
    out = []
    rest = value
    for i in range(count):
        digit = jnp.round(rest)
        out.append(digit.astype(BF16))
        rest = rest - digit
        if extra is not None and i == extra_at - 1:
            rest = rest + extra * (256.0 ** (extra_at - 1))
        rest = rest * 256.0
    return out


def levels_to_pair(levels):
    high = levels[-1]
    low = jnp.zeros_like(high)
    for level in reversed(levels[:-1]):
        high, err = two_sum(level, high * (1.0 / 256.0))
        low = low * (1.0 / 256.0) + err
    return high, low


def operator_kernel(k, nx, vec_ref, react_ref, low_ref, high_ref, inside_ref, table_ref, w_ref, gram_ref, field, react, both):
    halo = POWERS
    total = nx + 2 * halo
    for x in range(nx):
        field[halo + x] = vec_ref[:, x, :]
    for x in range(halo):
        field[x] = low_ref[:k, x, :]
        field[halo + nx + x] = high_ref[:k, x, :]
    react[0:halo] = low_ref[k]
    react[halo : halo + nx] = react_ref[...]
    react[halo + nx : total] = high_ref[k]
    low_inside = inside_ref[0]
    high_inside = inside_ref[1]
    table = table_ref[...]
    for step in range(POWERS):
        first, last = step, total - step

        def product(x, _):
            rows = field[x]
            one, two, three = split3(rows)
            both[x] = dot(one, table) + dot(two, table) + dot(three, table)
            return 0

        lax.fori_loop(first, last, product, 0)

        def combine(x, _):
            value = (
                both[x - 1, :, :PLANE] + both[x + 1, :, :PLANE] + both[x, :, PLANE:]
            ) * (1.0 / 216.0) + react[pl.ds(x, 1), :] * field[x]
            keep = jnp.where(x < halo, low_inside, jnp.where(x >= halo + nx, high_inside, 1.0))
            field[x] = value * keep
            return 0

        lax.fori_loop(first + 1, last - 1, combine, 0)
    peak = jnp.abs(field[halo])
    for x in range(1, nx):
        peak = jnp.maximum(peak, jnp.abs(field[halo + x]))
    peak = jnp.max(peak, axis=1, keepdims=True)
    size, inverse = power_below(peak)
    scale = inverse * 64.0
    slices = 4
    group = 4
    pairs = None
    for start in range(0, nx, group):
        parts = [[] for _ in range(slices)]
        for x in range(start, start + group):
            for s, digit in enumerate(digits(field[halo + x] * scale, slices)):
                parts[s].append(digit)
        stack = jnp.concatenate([jnp.concatenate(p, axis=1) for p in parts], axis=0)
        counts = dot_t(stack, stack)
        block = [[counts[i * k : (i + 1) * k, j * k : (j + 1) * k] for j in range(slices)] for i in range(slices)]
        tail = [
            sum(block[i][level - i] for i in range(slices) if 0 <= level - i < slices)
            for level in range(3, 2 * slices - 1)
        ]
        rest = tail[-1]
        for value in reversed(tail[:-1]):
            rest = value + rest * (1.0 / 256.0)
        terms = [
            rest * 2.0**-24,
            block[1][1] * 2.0**-16,
            (block[0][2] + block[2][0]) * 2.0**-16,
            block[0][1] * 2.0**-8,
            block[1][0] * 2.0**-8,
            block[0][0],
        ]
        for term in terms:
            if pairs is None:
                pairs = (term, jnp.zeros_like(term))
            else:
                high, err = two_sum(pairs[0], term)
                pairs = (high, pairs[1] + err)
    high, err = two_sum(pairs[0], pairs[1])
    row = size * (1.0 / 64.0)
    eye = lax.broadcasted_iota(jnp.int32, (k, k), 0) == lax.broadcasted_iota(jnp.int32, (k, k), 1)
    column = jnp.sum(jnp.where(eye, row, 0.0), axis=0, keepdims=True)
    gram_ref[:, 0, :] = jnp.concatenate([high * row * column, err * row * column], axis=1)
    for x in range(nx):
        w_ref[x] = field[halo + x]


def operator_and_gram(vectors, reaction, low, high, inside):
    k, nx, plane = vectors.shape
    total = nx + 2 * POWERS
    vmem = pl.BlockSpec(memory_space=pltpu.VMEM)
    smem = pl.BlockSpec(memory_space=pltpu.SMEM)
    return pl.pallas_call(
        lambda *refs: operator_kernel(k, nx, *refs),
        out_shape=(
            jax.ShapeDtypeStruct((nx, k, plane), F32),
            jax.ShapeDtypeStruct((k, 1, 2 * k), F32),
        ),
        in_specs=[vmem, vmem, vmem, vmem, smem, vmem],
        out_specs=(vmem, vmem),
        scratch_shapes=[
            pltpu.VMEM((total, k, plane), F32),
            pltpu.VMEM((total, plane), F32),
            pltpu.VMEM((total, k, 2 * plane), F32),
        ],
        name="operator_gram",
    )(vectors, reaction, low, high, inside, tables())


def pair_sum_kernel(parts_ref, out_ref):
    value = parts_ref[:, 0, :]
    width = value.shape[1]
    half = width // 2
    error = jnp.zeros_like(value)
    while value.shape[0] > 1:
        n = value.shape[0] // 2
        value, err = two_sum(value[:n], value[n:])
        error = error[:n] + error[n:] + err
    low = pltpu.roll(value, half, 1) + error
    high, err = two_sum(value, low)
    lane = lax.broadcasted_iota(jnp.int32, value.shape, 1)
    row = jnp.where(lane < half, high, pltpu.roll(err, half, 1))
    out_ref[:, 0, :] = jnp.broadcast_to(row, (out_ref.shape[0], width))


def pair_sum(parts, copies):
    return pl.pallas_call(
        pair_sum_kernel,
        out_shape=jax.ShapeDtypeStruct((copies, 1, parts.shape[2]), F32),
        in_specs=[pl.BlockSpec(memory_space=pltpu.VMEM)],
        out_specs=pl.BlockSpec(memory_space=pltpu.VMEM),
        name="pair_sum",
    )(parts)


def sum_over_devices(gram):
    near = lax.axis_size(NEAR)
    far = lax.axis_size(FAR)
    rows = lax.all_to_all(gram, NEAR, 0, 0)
    mine = pair_sum(rows, far)
    mine = pair_sum(lax.all_to_all(mine, FAR, 0, 0), near)
    return lax.all_to_all(mine, NEAR, 0, 0)


def level_sums(counts, k, rows, columns):
    out = []
    for level in range(rows + columns - 1):
        terms = [
            counts[i * k : (i + 1) * k, (level - i) * k : (level - i + 1) * k]
            for i in range(rows)
            if 0 <= level - i < columns
        ]
        total = terms[0]
        for term in terms[1:]:
            total = total + term
        out.append(total)
    return out


def whiten_kernel(gram_ref, guess_ref, gram_two_ref, exact_ref, product_ref):
    k = gram_ref.shape[0]
    pair = gram_ref[:, 0, :]
    high, low = pair[:, :k], pair[:, k:]
    eye = lax.broadcasted_iota(jnp.int32, (k, k), 0) == lax.broadcasted_iota(jnp.int32, (k, k), 1)
    diagonal = jnp.where(eye, high, 0.0)
    size_row, inverse_row = power_below(jnp.sum(diagonal, axis=0, keepdims=True), square=True)
    _, inverse_column = power_below(jnp.sum(diagonal, axis=1, keepdims=True), square=True)
    scale = inverse_column * inverse_row
    gram_digits = digits(high * scale * 32.0, 6, extra=low * scale * 32.0)
    guess = guess_ref[...] * size_row
    top, top_inverse = power_below(jnp.max(jnp.abs(guess), axis=1, keepdims=True))
    guess_digits = digits(guess * top_inverse * 64.0, 3)
    exact = sum(d.astype(F32) * 256.0**-i for i, d in enumerate(guess_digits))
    exact_ref[...] = exact * (top * (1.0 / 64.0)) * inverse_row
    guess_stack = jnp.concatenate(guess_digits, axis=0)
    counts = dot(guess_stack, jnp.concatenate(gram_digits, axis=1))
    high, low = levels_to_pair(level_sums(counts, k, 3, 6))
    product_ref[...] = (high + low) * (top * 2.0**-11) * size_row
    big, big_inverse = power_below(jnp.max(jnp.abs(high), axis=1, keepdims=True))
    product_digits = digits(high * big_inverse * 64.0, 6, extra=low * big_inverse * 64.0)
    counts = dot_t(jnp.concatenate(product_digits, axis=0), guess_stack)
    high, low = levels_to_pair(level_sums(counts, k, 6, 3))
    top_row = jnp.sum(jnp.where(eye, top, 0.0), axis=0, keepdims=True)
    gram_two_ref[...] = (high + low) * (top * 2.0**-11) * (big * (1.0 / 64.0)) * (top_row * (1.0 / 64.0))


def whiten(gram, guess):
    k = guess.shape[0]
    vmem = pl.BlockSpec(memory_space=pltpu.VMEM)
    square = jax.ShapeDtypeStruct((k, k), F32)
    return pl.pallas_call(
        whiten_kernel,
        out_shape=(square, square, square),
        in_specs=[vmem, vmem],
        out_specs=(vmem, vmem, vmem),
        name="whiten",
    )(gram, guess)


def lower_inverse(lower):
    eye = jnp.eye(lower.shape[0], dtype=F32)
    return lax.linalg.triangular_solve(lower, eye, left_side=True, lower=True)


def basis_kernel(scale, w_ref, factor_ref, rest_ref, out_ref):
    high, low = two_sum(factor_ref[...] * scale, rest_ref[...] * scale)
    p1, p2, p3 = split3(high)
    p4 = low.astype(BF16)
    left = jnp.concatenate([p1, p1, p1, p2, p2, p3, p4], axis=1)
    for x in range(w_ref.shape[0]):
        w1, w2, w3 = split3(w_ref[x])
        right = jnp.concatenate([w3, w2, w1, w2, w1, w1, w1], axis=0)
        out_ref[:, x, :] = dot(left, right)


def basis_of(w, factor, rest, scale):
    nx, k, plane = w.shape
    vmem = pl.BlockSpec(memory_space=pltpu.VMEM)
    return pl.pallas_call(
        lambda *refs: basis_kernel(scale, *refs),
        out_shape=jax.ShapeDtypeStruct((k, nx, plane), F32),
        in_specs=[vmem, vmem, vmem],
        out_specs=vmem,
        name="basis",
    )(w, factor, rest)


def per_device(vectors, reaction):
    k, nx, plane = vectors.shape
    peers = lax.axis_size(SFC_SUB)
    me = lax.axis_index(SFC_SUB)
    up = [(i, i + 1) for i in range(peers - 1)]
    down = [(i + 1, i) for i in range(peers - 1)]
    last = jnp.concatenate([vectors[:, nx - POWERS :], reaction[None, nx - POWERS :]], axis=0)
    leading = jnp.concatenate([vectors[:, :POWERS], reaction[None, :POWERS]], axis=0)
    low = lax.ppermute(last, SFC_SUB, up)
    high = lax.ppermute(leading, SFC_SUB, down)
    inside = jnp.stack([me > 0, me < peers - 1]).astype(F32)
    w, gram = operator_and_gram(vectors, reaction, low, high, inside)
    gram = sum_over_devices(gram)
    guess = lower_inverse(jnp.linalg.cholesky(gram[:, 0, :k]))
    gram_two, exact, product = whiten(gram, guess)
    second = lower_inverse(jnp.linalg.cholesky(gram_two))
    eye = jnp.eye(k, dtype=F32)
    rest = jnp.dot(second - eye, exact, precision=HIGHEST)
    scale = math.sqrt(peers * nx * plane)
    upper = jnp.triu(jnp.dot(second, product, precision=HIGHEST)) / scale
    return basis_of(w, exact, rest, scale), upper


def solution(mesh):
    torus = Mesh(mesh.devices.reshape(16, 8, 4, 2), ("sfc_0", "sfc_1", "sub_0", "sub_1"))
    in_specs = (P(None, SFC_SUB, None), P(SFC_SUB, None))
    out_specs = (P(None, SFC_SUB, None), P())
    return jax.shard_map(
        per_device, mesh=torus, in_specs=in_specs, out_specs=out_specs, check_vma=False
    )
```

```python
import math

import jax
import jax.numpy as jnp
import numpy as np
from jax import lax
from jax.experimental import pallas as pl
from jax.experimental.pallas import tpu as pltpu
from jax.sharding import Mesh
from jax.sharding import PartitionSpec as P

NY = 32
NL = 8
PLANE = NY * NL
POWERS = 3
SFC_SUB = ("sfc_0", "sfc_1", "sub_0", "sub_1")
FAR = ("sfc_0",)
NEAR = ("sfc_1", "sub_0", "sub_1")
DELTA_MASS = 0.5
F32 = jnp.float32
BF16 = jnp.bfloat16
HIGHEST = lax.Precision.HIGHEST


def line_tables(count):
    index = np.arange(count)
    offset = index[:, None] - index[None, :]
    near = (np.abs(offset) == 1).astype(np.float32)
    same = (offset == 0).astype(np.float32)
    return 4.0 * same + near, 2.0 * same - near


def tables():
    mass_across, stiff_across = line_tables(NY)
    mass_layers, stiff_layers = line_tables(NL)
    mass = np.kron(mass_layers, mass_across)
    stiff = (
        6.0 * (np.kron(mass_layers, stiff_across) + np.kron(stiff_layers, mass_across))
        + DELTA_MASS * mass
    )
    return np.concatenate([stiff - 6.0 * mass, 4.0 * stiff + 12.0 * mass], axis=1).astype(BF16)


def split3(value):
    one = value.astype(BF16)
    rest = value - one.astype(F32)
    two = rest.astype(BF16)
    three = (rest - two.astype(F32)).astype(BF16)
    return one, two, three


def dot(a, b):
    return lax.dot_general(a, b, (((1,), (0,)), ((), ())), preferred_element_type=F32)


def dot_t(a, b):
    return lax.dot_general(a, b, (((1,), (1,)), ((), ())), preferred_element_type=F32)


def two_sum(a, b):
    s = a + b
    t = s - a
    return s, (a - (s - t)) + (b - t)


def power_below(x, square=False):
    low = -60 if square else -120
    p = jnp.full_like(x, 2.0**low)
    q = jnp.full_like(x, 2.0**-low)
    for k in (64, 32, 16, 8, 4, 2, 1) if square else (128, 64, 32, 16, 8, 4, 2, 1):
        half = 2.0 ** (k // 2) if k > 1 else 2.0
        up = p * half * (half if k > 1 else 1.0)
        down = q * (1.0 / half) * (1.0 / half if k > 1 else 1.0)
        fits = (up * up if square else up) <= x
        p, q = jnp.where(fits, up, p), jnp.where(fits, down, q)
    return p, q


def digits(value, count, extra=None, extra_at=3):
    out = []
    rest = value
    for i in range(count):
        digit = jnp.round(rest)
        out.append(digit.astype(BF16))
        rest = rest - digit
        if extra is not None and i == extra_at - 1:
            rest = rest + extra * (256.0 ** (extra_at - 1))
        rest = rest * 256.0
    return out


def levels_to_pair(levels):
    high = levels[-1]
    low = jnp.zeros_like(high)
    for level in reversed(levels[:-1]):
        high, err = two_sum(level, high * (1.0 / 256.0))
        low = low * (1.0 / 256.0) + err
    return high, low


def operator_kernel(k, nx, vec_ref, react_ref, low_ref, high_ref, inside_ref, table_ref, w_ref, gram_ref, field, react, both):
    halo = POWERS
    total = nx + 2 * halo
    chunk = 2
    for x in range(nx):
        field[halo + x] = vec_ref[:, x, :]
    for x in range(halo):
        field[x] = low_ref[x, :k, :]
        field[halo + nx + x] = high_ref[x, :k, :]
    table = table_ref[...]
    react[0:halo] = low_ref[:, k, :]
    react[halo : halo + nx] = react_ref[...]
    react[halo + nx : total] = high_ref[:, k, :]
    low_inside = inside_ref[0]
    high_inside = inside_ref[1]
    for step in range(POWERS):
        first, last = step, total - step
        chunk = (22,20,18)[step]

        def product(i, _):
            x = first + chunk * i
            one, two, three = split3(field[pl.ds(x, chunk)].reshape(chunk * k, PLANE))
            parts = dot(jnp.concatenate([one, two, three], axis=0), table)
            n = chunk * k
            both[pl.ds(x, chunk)] = (parts[:n] + parts[n : 2 * n] + parts[2 * n :]).reshape(chunk, k, 2 * PLANE)
            return 0

        lax.fori_loop(0, (last - first) // chunk, product, 0)

        def combine(x, _):
            value = (
                both[x - 1, :, :PLANE] + both[x + 1, :, :PLANE] + both[x, :, PLANE:]
            ) * (1.0 / 216.0) + react[pl.ds(x, 1), :] * field[x]
            if step < POWERS - 1:
                keep = jnp.where(x < halo, low_inside, jnp.where(x >= halo + nx, high_inside, 1.0))
                field[x] = value * keep
            else:
                w_ref[x - halo] = value
            return 0

        lax.fori_loop(first + 1, last - 1, combine, 0, unroll=4)
    peak = jnp.abs(w_ref[0])
    for x in range(1, nx):
        peak = jnp.maximum(peak, jnp.abs(w_ref[x]))
    peak = jnp.max(peak, axis=1, keepdims=True)
    size, inverse = power_below(peak)
    scale = inverse * 64.0
    slices = 4
    group = 4
    pairs = None
    for start in range(0, nx, group):
        parts = [[] for _ in range(slices)]
        for x in range(start, start + group):
            for s, digit in enumerate(digits(w_ref[x] * scale, slices)):
                parts[s].append(digit)
        stack = jnp.concatenate([jnp.concatenate(p, axis=1) for p in parts], axis=0)
        counts = dot_t(stack, stack)
        block = [[counts[i * k : (i + 1) * k, j * k : (j + 1) * k] for j in range(slices)] for i in range(slices)]
        tail = [
            sum(block[i][level - i] for i in range(slices) if 0 <= level - i < slices)
            for level in range(3, 2 * slices - 1)
        ]
        rest = tail[-1]
        for value in reversed(tail[:-1]):
            rest = value + rest * (1.0 / 256.0)
        terms = [
            rest * 2.0**-24,
            block[1][1] * 2.0**-16,
            (block[0][2] + block[2][0]) * 2.0**-16,
            block[0][1] * 2.0**-8,
            block[1][0] * 2.0**-8,
            block[0][0],
        ]
        for term in terms:
            if pairs is None:
                pairs = (term, jnp.zeros_like(term))
            else:
                high, err = two_sum(pairs[0], term)
                pairs = (high, pairs[1] + err)
    high, err = two_sum(pairs[0], pairs[1])
    row = size * (1.0 / 64.0)
    eye = lax.broadcasted_iota(jnp.int32, (k, k), 0) == lax.broadcasted_iota(jnp.int32, (k, k), 1)
    column = jnp.sum(jnp.where(eye, row, 0.0), axis=0, keepdims=True)
    gram_ref[:, 0, :] = jnp.concatenate([high * row * column, err * row * column], axis=1)


def operator_and_gram(vectors, reaction, low, high, inside):
    k, nx, plane = vectors.shape
    total = nx + 2 * POWERS
    vmem = pl.BlockSpec(memory_space=pltpu.VMEM)
    smem = pl.BlockSpec(memory_space=pltpu.SMEM)
    return pl.pallas_call(
        lambda *refs: operator_kernel(k, nx, *refs),
        out_shape=(
            jax.ShapeDtypeStruct((nx, k, plane), F32),
            jax.ShapeDtypeStruct((k, 1, 2 * k), F32),
        ),
        in_specs=[vmem, vmem, vmem, vmem, smem, vmem],
        out_specs=(vmem, vmem),
        scratch_shapes=[
            pltpu.VMEM((total, k, plane), F32),
            pltpu.VMEM((total, plane), F32),
            pltpu.VMEM((total, k, 2 * plane), F32),
        ],
        name="operator_gram",
    )(vectors, reaction, low, high, inside, jnp.asarray(tables()))


def pair_sum_kernel(parts_ref, out_ref):
    value = parts_ref[:, 0, :]
    width = value.shape[1]
    half = width // 2
    error = jnp.zeros_like(value)
    while value.shape[0] > 1:
        n = value.shape[0] // 2
        value, err = two_sum(value[:n], value[n:])
        error = error[:n] + error[n:] + err
    low = pltpu.roll(value, half, 1) + error
    high, err = two_sum(value, low)
    lane = lax.broadcasted_iota(jnp.int32, value.shape, 1)
    row = jnp.where(lane < half, high, pltpu.roll(err, half, 1))
    out_ref[:, 0, :] = jnp.broadcast_to(row, (out_ref.shape[0], width))


def pair_sum(parts, copies):
    return pl.pallas_call(
        pair_sum_kernel,
        out_shape=jax.ShapeDtypeStruct((copies, 1, parts.shape[2]), F32),
        in_specs=[pl.BlockSpec(memory_space=pltpu.VMEM)],
        out_specs=pl.BlockSpec(memory_space=pltpu.VMEM),
        name="pair_sum",
    )(parts)


def sum_over_devices(gram):
    near = lax.axis_size(NEAR)
    far = lax.axis_size(FAR)
    rows = lax.all_to_all(gram, NEAR, 0, 0)
    mine = pair_sum(rows, far)
    mine = pair_sum(lax.all_to_all(mine, FAR, 0, 0), near)
    return lax.all_to_all(mine, NEAR, 0, 0)


def level_sums(counts, k, rows, columns):
    out = []
    for level in range(rows + columns - 1):
        terms = [
            counts[i * k : (i + 1) * k, (level - i) * k : (level - i + 1) * k]
            for i in range(rows)
            if 0 <= level - i < columns
        ]
        total = terms[0]
        for term in terms[1:]:
            total = total + term
        out.append(total)
    return out


def dot_of_stack(a_parts, b_parts):
    return dot(jnp.concatenate(a_parts, axis=1), jnp.concatenate(b_parts, axis=0))


def dot_full(a, b):
    a1, a2, a3 = split3(a)
    b1, b2, b3 = split3(b)
    return dot_of_stack([a1, a1, a2, a1, a2, a3], [b1, b2, b1, b3, b2, b1])


def eliminate(square):
    k = square.shape[0]
    row = lax.broadcasted_iota(jnp.int32, (k, 2 * k), 0)
    lane = lax.broadcasted_iota(jnp.int32, (k, 2 * k), 1)
    eye = (row[:, :k] == lane[:, :k]).astype(F32)
    block = 8
    work = jnp.concatenate([square, eye], axis=1)
    done = []
    for start in range(0, k, block):
        rows = work.shape[0]
        columns = [jnp.broadcast_to(work[:, start + a : start + a + 1], (rows, 2 * k)) for a in range(block)]
        below = lax.broadcasted_iota(jnp.int32, (rows, 2 * k), 0)
        for a in range(block):
            inverse = 1.0 / columns[a][a : a + 1, :]
            many = jnp.where(below > a, columns[a] * inverse, 0.0)
            for b in range(a + 1, block):
                columns[b] = columns[b] - many * columns[b][a : a + 1, :]
            work = work - many * work[a : a + 1, :]
        done.append(work[:block])
        work = work[block:]
    work = jnp.concatenate(done, axis=0)
    pivot = jnp.sum(work[:, :k] * eye, axis=1, keepdims=True)
    return work[:, k:] * lax.rsqrt(pivot)


def near_identity(delta, strict, half):
    def lower(value):
        return jnp.where(strict, value, jnp.where(half, 0.5 * value, 0.0))

    y = -lower(delta)
    for _ in range(3):
        a = dot_full(y, delta)
        outer = y + a
        y1, y2, y3 = split3(y)
        o1, o2, o3 = split3(outer)
        square = dot_t(
            jnp.concatenate([o1, o1, o2, o1, o2, o3], axis=1), jnp.concatenate([y1, y2, y1, y3, y2, y1], axis=1)
        )
        error = lower(delta + (y + y.T) + (a + a.T) + square)
        y = y - error - dot_full(error, y)
    return y


def factor_kernel(scale, gram_ref, high_ref, low_ref, upper_ref, y_ref):
    k = gram_ref.shape[0]
    pair = gram_ref[:, 0, :]
    high, low = pair[:, :k], pair[:, k:]
    row = lax.broadcasted_iota(jnp.int32, (k, k), 0)
    lane = lax.broadcasted_iota(jnp.int32, (k, k), 1)
    eye = row == lane
    diagonal = jnp.where(eye, high, 0.0)
    size_row, inverse_row = power_below(jnp.sum(diagonal, axis=0, keepdims=True), square=True)
    _, inverse_column = power_below(jnp.sum(diagonal, axis=1, keepdims=True), square=True)
    unit = inverse_column * inverse_row
    high = high * unit
    low = low * unit
    gram_digits = digits(high * 32.0, 6, extra=low * 32.0)
    guess = eliminate(high)
    top, top_inverse = power_below(jnp.max(jnp.abs(guess), axis=1, keepdims=True))
    guess_digits = digits(guess * top_inverse * 64.0, 3)
    exact = sum(d.astype(F32) * 256.0**-i for i, d in enumerate(guess_digits))
    exact = exact * (top * (1.0 / 64.0))
    guess_stack = jnp.concatenate(guess_digits, axis=0)
    counts = dot(guess_stack, jnp.concatenate(gram_digits, axis=1))
    high, low = levels_to_pair(level_sums(counts, k, 3, 6))
    product = (high + low) * (top * 2.0**-11)
    big, big_inverse = power_below(jnp.max(jnp.abs(high), axis=1, keepdims=True))
    product_digits = digits(high * big_inverse * 64.0, 6, extra=low * big_inverse * 64.0)
    counts = dot_t(jnp.concatenate(product_digits, axis=0), guess_stack)
    high, low = levels_to_pair(level_sums(counts, k, 6, 3))
    top_row = jnp.sum(jnp.where(eye, top, 0.0), axis=0, keepdims=True)
    unit = (top * 2.0**-11) * (big * (1.0 / 64.0)) * (top_row * (1.0 / 64.0))
    high = high * unit
    low = low * unit
    delta = jnp.where(eye, high - 1.0, high) + low
    worst = jnp.max(jnp.abs(delta))
    small = worst < 2.0**-8

    @pl.when(small)
    def _():
        y_ref[...] = near_identity(delta, row > lane, eye)

    @pl.when(jnp.logical_not(small))
    def _():
        y_ref[...] = eliminate(high + low) - eye.astype(F32)

    y = y_ref[...]
    rest = dot_full(y, exact)
    high, low = two_sum(exact, rest)
    unit = inverse_row * scale
    high_ref[...] = high * unit
    low_ref[...] = low * unit
    upper = product + dot_full(y, product)
    upper_ref[...] = jnp.where(row <= lane, upper, 0.0) * (size_row * (1.0 / scale))


def factor(gram, scale):
    k = gram.shape[0]
    vmem = pl.BlockSpec(memory_space=pltpu.VMEM)
    square = jax.ShapeDtypeStruct((k, k), F32)
    return pl.pallas_call(
        lambda *refs: factor_kernel(scale, *refs),
        out_shape=(square, square, square),
        in_specs=[vmem],
        out_specs=(vmem, vmem, vmem),
        scratch_shapes=[pltpu.VMEM((k, k), F32)],
        name="factor",
    )(gram)


def basis_kernel(w_ref, high_ref, low_ref, out_ref):
    p1, p2, p3 = split3(high_ref[...])
    p4 = low_ref[...].astype(BF16)
    left = jnp.concatenate([p1, p1, p1, p2, p2, p3, p4], axis=1)
    for x in range(w_ref.shape[0]):
        w1, w2, w3 = split3(w_ref[x])
        right = jnp.concatenate([w3, w2, w1, w2, w1, w1, w1], axis=0)
        out_ref[:, x, :] = dot(left, right)


def basis_of(w, high, low):
    nx, k, plane = w.shape
    vmem = pl.BlockSpec(memory_space=pltpu.VMEM)
    return pl.pallas_call(
        basis_kernel,
        out_shape=jax.ShapeDtypeStruct((k, nx, plane), F32),
        in_specs=[vmem, vmem, vmem],
        out_specs=vmem,
        name="basis",
    )(w, high, low)


def border(vectors, reaction):
    rows = jnp.swapaxes(vectors, 0, 1)
    react = jnp.broadcast_to(reaction[:, None], (reaction.shape[0], 8, reaction.shape[1]))
    return jnp.concatenate([rows, react], axis=1)


def per_device(vectors, reaction):
    k, nx, plane = vectors.shape
    peers = lax.axis_size(SFC_SUB)
    me = lax.axis_index(SFC_SUB)
    up = [(i, i + 1) for i in range(peers - 1)]
    down = [(i + 1, i) for i in range(peers - 1)]
    last = border(vectors[:, nx - POWERS :], reaction[nx - POWERS :])
    leading = border(vectors[:, :POWERS], reaction[:POWERS])
    low = lax.ppermute(last, SFC_SUB, up)
    high = lax.ppermute(leading, SFC_SUB, down)
    inside = jnp.stack([me > 0, me < peers - 1]).astype(F32)
    w, gram = operator_and_gram(vectors, reaction, low, high, inside)
    gram = sum_over_devices(gram)
    high, low, upper = factor(gram, math.sqrt(peers * nx * plane))
    return basis_of(w, high, low), upper


def solution(mesh):
    torus = Mesh(mesh.devices.reshape(16, 8, 4, 2), ("sfc_0", "sfc_1", "sub_0", "sub_1"))
    in_specs = (P(None, SFC_SUB, None), P(SFC_SUB, None))
    out_specs = (P(None, SFC_SUB, None), P())
    return jax.shard_map(
        per_device, mesh=torus, in_specs=in_specs, out_specs=out_specs, check_vma=False
    )
```

```python
import math

import jax
import jax.numpy as jnp
import numpy as np
from jax import lax
from jax.experimental import pallas as pl
from jax.experimental.pallas import tpu as pltpu
from jax.sharding import Mesh
from jax.sharding import PartitionSpec as P

NY = 32
NL = 8
PLANE = NY * NL
POWERS = 3
SFC_SUB = ("sfc_0", "sfc_1", "sub_0", "sub_1")
FAR = ("sfc_0",)
NEAR = ("sfc_1", "sub_0", "sub_1")
DELTA_MASS = 0.5
F32 = jnp.float32
BF16 = jnp.bfloat16


SMALL = pltpu.CompilerParams(vmem_limit_bytes=24 * 2**20)
VMEM_SPEC = pl.BlockSpec(memory_space=pltpu.VMEM)


def in_vmem(*shape):
    return pltpu.VMEM(shape, F32)


def vmem(array):
    return pltpu.with_memory_space_constraint(array, pltpu.VMEM)


def line_tables(count):
    index = np.arange(count)
    offset = index[:, None] - index[None, :]
    near = (np.abs(offset) == 1).astype(np.float32)
    same = (offset == 0).astype(np.float32)
    return 4.0 * same + near, 2.0 * same - near


def tables():
    mass_across, stiff_across = line_tables(NY)
    mass_layers, stiff_layers = line_tables(NL)
    mass = np.kron(mass_layers, mass_across)
    stiff = (
        6.0 * (np.kron(mass_layers, stiff_across) + np.kron(stiff_layers, mass_across))
        + DELTA_MASS * mass
    )
    return np.concatenate([stiff - 6.0 * mass, 4.0 * stiff + 12.0 * mass], axis=1).astype(BF16)


def split3(value):
    one = value.astype(BF16)
    rest = value - one.astype(F32)
    two = rest.astype(BF16)
    three = (rest - two.astype(F32)).astype(BF16)
    return one, two, three


def dot(a, b):
    return lax.dot_general(a, b, (((1,), (0,)), ((), ())), preferred_element_type=F32)


def dot_t(a, b):
    return lax.dot_general(a, b, (((1,), (1,)), ((), ())), preferred_element_type=F32)


def two_sum(a, b):
    s = a + b
    t = s - a
    return s, (a - (s - t)) + (b - t)


def power_below(x, square=False):
    low = -60 if square else -120
    p = jnp.full_like(x, 2.0**low)
    q = jnp.full_like(x, 2.0**-low)
    for k in (64, 32, 16, 8, 4, 2, 1) if square else (128, 64, 32, 16, 8, 4, 2, 1):
        half = 2.0 ** (k // 2) if k > 1 else 2.0
        up = p * half * (half if k > 1 else 1.0)
        down = q * (1.0 / half) * (1.0 / half if k > 1 else 1.0)
        fits = (up * up if square else up) <= x
        p, q = jnp.where(fits, up, p), jnp.where(fits, down, q)
    return p, q


def digits(value, count, extra=None, extra_at=3):
    out = []
    rest = value
    for i in range(count):
        digit = jnp.round(rest)
        out.append(digit.astype(BF16))
        rest = rest - digit
        if extra is not None and i == extra_at - 1:
            rest = rest + extra * (256.0 ** (extra_at - 1))
        rest = rest * 256.0
    return out


def levels_to_pair(levels):
    high = levels[-1]
    low = jnp.zeros_like(high)
    for level in reversed(levels[:-1]):
        high, err = two_sum(level, high * (1.0 / 256.0))
        low = low * (1.0 / 256.0) + err
    return high, low


def border_kernel(odd_ref, vec_ref, react_ref, inner_ref, outer_ref):
    k, nx, plane = vec_ref.shape
    odd = odd_ref[0]

    def fill(ref, start):
        for j in range(POWERS):
            ref[j, :k, :] = vec_ref[:, start + j, :]
            ref[j, k:, :] = jnp.broadcast_to(react_ref[start + j : start + j + 1, :], (8, plane))

    @pl.when(odd == 0)
    def _():
        fill(inner_ref, nx - POWERS)
        fill(outer_ref, 0)

    @pl.when(odd != 0)
    def _():
        fill(inner_ref, 0)
        fill(outer_ref, nx - POWERS)


def borders(odd, vectors, reaction):
    k, nx, plane = vectors.shape
    shape = in_vmem(POWERS, k + 8, plane)
    return pl.pallas_call(
        border_kernel,
        out_shape=(shape, shape),
        in_specs=[pl.BlockSpec(memory_space=pltpu.SMEM), VMEM_SPEC, VMEM_SPEC],
        out_specs=(VMEM_SPEC, VMEM_SPEC),
        compiler_params=SMALL,
        name="borders",
    )(odd, vectors, reaction)


def products(field, both, table, start, count):
    k = field.shape[1]
    n = count * k
    one, two, three = split3(field[pl.ds(start, count)].reshape(n, PLANE))
    parts = dot(jnp.concatenate([one, two, three], axis=0), table)
    both[pl.ds(start, count)] = (parts[:n] + parts[n : 2 * n] + parts[2 * n :]).reshape(count, k, 2 * PLANE)


def begin_kernel(vec_ref, table_ref, field, both):
    k, nx, plane = vec_ref.shape
    for x in range(nx):
        field[x] = vec_ref[:, x, :]
    table = table_ref[...]

    def one_part(i, _):
        products(field, both, table, 0, nx)
        return 0

    lax.fori_loop(0, 1, one_part, 0)


def begin(vectors, table):
    k, nx, plane = vectors.shape
    return pl.pallas_call(
        begin_kernel,
        out_shape=(in_vmem(nx, k, plane), in_vmem(nx, k, 2 * plane)),
        in_specs=[VMEM_SPEC, VMEM_SPEC],
        out_specs=(VMEM_SPEC, VMEM_SPEC),
        cost_estimate=pl.CostEstimate(flops=2 * 3 * nx * k * plane * 2 * plane, bytes_accessed=0, transcendentals=0),
        compiler_params=SMALL,
        name="begin",
    )(vectors, table)


def operator_kernel(k, nx, flags_ref, react_ref, inner_ref, outer_ref, table_ref, own_ref, own_both_ref, w_ref, gram_ref, field, both, react):
    halo = POWERS
    total = nx + 2 * halo
    odd = flags_ref[0]
    low_inside = flags_ref[1].astype(F32)
    high_inside = flags_ref[2].astype(F32)
    react[halo : halo + nx] = react_ref[...]

    def fill(low_ref, high_ref):
        field[0:halo] = low_ref[:, :k, :]
        field[halo + nx : total] = high_ref[:, :k, :]
        react[0:halo] = low_ref[:, k, :]
        react[halo + nx : total] = high_ref[:, k, :]

    @pl.when(odd == 0)
    def _():
        fill(outer_ref, inner_ref)

    @pl.when(odd != 0)
    def _():
        fill(inner_ref, outer_ref)

    table = table_ref[...]

    def combine(step, x, values, parts, offset):
        value = (
            parts[x - 1 - offset, :, :PLANE] + parts[x + 1 - offset, :, :PLANE] + parts[x - offset, :, PLANE:]
        ) * (1.0 / 216.0) + react[pl.ds(x, 1), :] * values[x - offset]
        if step < POWERS - 1:
            keep = jnp.where(x < halo, low_inside, jnp.where(x >= halo + nx, high_inside, 1.0))
            field[x] = value * keep
        else:
            w_ref[x - halo] = value
        return 0

    def edge(i, _):
        products(field, both, table, i * (halo + nx), halo)
        return 0

    lax.fori_loop(0, 2, edge, 0)

    def own_edge(i, _):
        x = jnp.where(i < 2, i, nx - 4 + i)
        field[halo + x] = own_ref[x]
        both[halo + x] = own_both_ref[x]
        return 0

    lax.fori_loop(0, 4, own_edge, 0)

    def outside(i, _):
        x = jnp.where(i < halo, 1 + i, nx - 1 + i)
        return combine(0, x, field, both, 0)

    lax.fori_loop(0, 2 * halo, outside, 0)

    def inside(x, _):
        return combine(0, x, own_ref, own_both_ref, halo)

    lax.fori_loop(halo + 1, halo + nx - 1, inside, 0, unroll=7)
    for step in range(1, POWERS):
        first, last = step, total - step

        def product(i, _):
            products(field, both, table, first, last - first)
            return 0

        lax.fori_loop(0, 1, product, 0)

        def later(x, _):
            return combine(step, x, field, both, 0)

        lax.fori_loop(first + 1, last - 1, later, 0, unroll=(last - first - 2) // 2)
    peak = jnp.abs(w_ref[0])
    for x in range(1, nx):
        peak = jnp.maximum(peak, jnp.abs(w_ref[x]))
    peak = jnp.max(peak, axis=1, keepdims=True)
    size, inverse = power_below(peak)
    scale = inverse * 64.0
    slices = 4
    group = 4
    pairs = None
    for start in range(0, nx, group):
        parts = [[] for _ in range(slices)]
        for x in range(start, start + group):
            for s, digit in enumerate(digits(w_ref[x] * scale, slices)):
                parts[s].append(digit)
        stack = jnp.concatenate([jnp.concatenate(p, axis=1) for p in parts], axis=0)
        counts = dot_t(stack, stack)
        block = [[counts[i * k : (i + 1) * k, j * k : (j + 1) * k] for j in range(slices)] for i in range(slices)]
        tail = [
            sum(block[i][level - i] for i in range(slices) if 0 <= level - i < slices)
            for level in range(3, 2 * slices - 1)
        ]
        rest = tail[-1]
        for value in reversed(tail[:-1]):
            rest = value + rest * (1.0 / 256.0)
        terms = [
            rest * 2.0**-24,
            block[1][1] * 2.0**-16,
            (block[0][2] + block[2][0]) * 2.0**-16,
            block[0][1] * 2.0**-8,
            block[1][0] * 2.0**-8,
            block[0][0],
        ]
        for term in terms:
            if pairs is None:
                pairs = (term, jnp.zeros_like(term))
            else:
                high, err = two_sum(pairs[0], term)
                pairs = (high, pairs[1] + err)
    high, err = two_sum(pairs[0], pairs[1])
    row = size * (1.0 / 64.0)
    eye = lax.broadcasted_iota(jnp.int32, (k, k), 0) == lax.broadcasted_iota(jnp.int32, (k, k), 1)
    column = jnp.sum(jnp.where(eye, row, 0.0), axis=0, keepdims=True)
    gram_ref[:, 0, :] = jnp.concatenate([high * row * column, err * row * column], axis=1)


def operator_and_gram(flags, reaction, inner, outer, table, own, own_both):
    nx, k, plane = own.shape
    total = nx + 2 * POWERS
    smem = pl.BlockSpec(memory_space=pltpu.SMEM)
    return pl.pallas_call(
        lambda *refs: operator_kernel(k, nx, *refs),
        out_shape=(in_vmem(nx, k, plane), in_vmem(k, 1, 2 * k)),
        in_specs=[smem] + [VMEM_SPEC] * 6,
        out_specs=(VMEM_SPEC, VMEM_SPEC),
        scratch_shapes=[
            pltpu.VMEM((total, k, plane), F32),
            pltpu.VMEM((total, k, 2 * plane), F32),
            pltpu.VMEM((total, plane), F32),
        ],
        cost_estimate=pl.CostEstimate(flops=2 * 3 * 44 * k * plane * 2 * plane, bytes_accessed=0, transcendentals=0),
        compiler_params=SMALL,
        name="operator_gram",
    )(flags, reaction, vmem(inner), vmem(outer), table, vmem(own), vmem(own_both))


def pair_sum_kernel(parts_ref, out_ref):
    value = parts_ref[:, 0, :]
    width = value.shape[1]
    half = width // 2
    error = jnp.zeros_like(value)
    while value.shape[0] > 1:
        n = value.shape[0] // 2
        value, err = two_sum(value[:n], value[n:])
        error = error[:n] + error[n:] + err
    low = pltpu.roll(value, half, 1) + error
    high, err = two_sum(value, low)
    lane = lax.broadcasted_iota(jnp.int32, value.shape, 1)
    row = jnp.where(lane < half, high, pltpu.roll(err, half, 1))
    out_ref[:, 0, :] = jnp.broadcast_to(row, (out_ref.shape[0], width))


def pair_sum(parts, copies):
    return pl.pallas_call(
        pair_sum_kernel,
        out_shape=in_vmem(copies, 1, parts.shape[2]),
        in_specs=[VMEM_SPEC],
        out_specs=VMEM_SPEC,
        compiler_params=SMALL,
        name="pair_sum",
    )(vmem(parts))


def sum_over_devices(gram):
    near = lax.axis_size(NEAR)
    far = lax.axis_size(FAR)
    rows = lax.all_to_all(gram, NEAR, 0, 0)
    mine = pair_sum(rows, far)
    mine = pair_sum(lax.all_to_all(mine, FAR, 0, 0), near)
    return lax.all_to_all(mine, NEAR, 0, 0)


def level_sums(counts, k, rows, columns):
    out = []
    for level in range(rows + columns - 1):
        terms = [
            counts[i * k : (i + 1) * k, (level - i) * k : (level - i + 1) * k]
            for i in range(rows)
            if 0 <= level - i < columns
        ]
        total = terms[0]
        for term in terms[1:]:
            total = total + term
        out.append(total)
    return out


def dot_of_stack(a_parts, b_parts):
    return dot(jnp.concatenate(a_parts, axis=1), jnp.concatenate(b_parts, axis=0))


def dot_full(a, b):
    a1, a2, a3 = split3(a)
    b1, b2, b3 = split3(b)
    return dot_of_stack([a1, a1, a2, a1, a2, a3], [b1, b2, b1, b3, b2, b1])


def eliminate(square):
    k = square.shape[0]
    row = lax.broadcasted_iota(jnp.int32, (k, 2 * k), 0)
    lane = lax.broadcasted_iota(jnp.int32, (k, 2 * k), 1)
    eye = (row[:, :k] == lane[:, :k]).astype(F32)
    block = 8
    work = jnp.concatenate([square, eye], axis=1)
    done = []
    for start in range(0, k, block):
        rows = work.shape[0]
        columns = [jnp.broadcast_to(work[:, start + a : start + a + 1], (rows, 2 * k)) for a in range(block)]
        below = lax.broadcasted_iota(jnp.int32, (rows, 2 * k), 0)
        for a in range(block):
            inverse = 1.0 / columns[a][a : a + 1, :]
            many = jnp.where(below > a, columns[a] * inverse, 0.0)
            for b in range(a + 1, block):
                columns[b] = columns[b] - many * columns[b][a : a + 1, :]
            work = work - many * work[a : a + 1, :]
        done.append(work[:block])
        work = work[block:]
    work = jnp.concatenate(done, axis=0)
    pivot = jnp.sum(work[:, :k] * eye, axis=1, keepdims=True)
    return work[:, k:] * lax.rsqrt(pivot)


def near_identity(delta, strict, half):
    def lower(value):
        return jnp.where(strict, value, jnp.where(half, 0.5 * value, 0.0))

    y = -lower(delta)
    for _ in range(3):
        a = dot_full(y, delta)
        outer = y + a
        y1, y2, y3 = split3(y)
        o1, o2, o3 = split3(outer)
        square = dot_t(
            jnp.concatenate([o1, o1, o2, o1, o2, o3], axis=1), jnp.concatenate([y1, y2, y1, y3, y2, y1], axis=1)
        )
        error = lower(delta + (y + y.T) + (a + a.T) + square)
        y = y - error - dot_full(error, y)
    return y


def factor_kernel(scale, gram_ref, high_ref, low_ref, upper_ref, y_ref):
    k = gram_ref.shape[0]
    pair = gram_ref[:, 0, :]
    high, low = pair[:, :k], pair[:, k:]
    row = lax.broadcasted_iota(jnp.int32, (k, k), 0)
    lane = lax.broadcasted_iota(jnp.int32, (k, k), 1)
    eye = row == lane
    diagonal = jnp.where(eye, high, 0.0)
    size_row, inverse_row = power_below(jnp.sum(diagonal, axis=0, keepdims=True), square=True)
    _, inverse_column = power_below(jnp.sum(diagonal, axis=1, keepdims=True), square=True)
    unit = inverse_column * inverse_row
    high = high * unit
    low = low * unit
    gram_digits = digits(high * 32.0, 6, extra=low * 32.0)
    guess = eliminate(high)
    top, top_inverse = power_below(jnp.max(jnp.abs(guess), axis=1, keepdims=True))
    guess_digits = digits(guess * top_inverse * 64.0, 3)
    exact = sum(d.astype(F32) * 256.0**-i for i, d in enumerate(guess_digits))
    exact = exact * (top * (1.0 / 64.0))
    guess_stack = jnp.concatenate(guess_digits, axis=0)
    counts = dot(guess_stack, jnp.concatenate(gram_digits, axis=1))
    high, low = levels_to_pair(level_sums(counts, k, 3, 6))
    product = (high + low) * (top * 2.0**-11)
    big, big_inverse = power_below(jnp.max(jnp.abs(high), axis=1, keepdims=True))
    product_digits = digits(high * big_inverse * 64.0, 6, extra=low * big_inverse * 64.0)
    counts = dot_t(jnp.concatenate(product_digits, axis=0), guess_stack)
    high, low = levels_to_pair(level_sums(counts, k, 6, 3))
    top_row = jnp.sum(jnp.where(eye, top, 0.0), axis=0, keepdims=True)
    unit = (top * 2.0**-11) * (big * (1.0 / 64.0)) * (top_row * (1.0 / 64.0))
    high = high * unit
    low = low * unit
    delta = jnp.where(eye, high - 1.0, high) + low
    worst = jnp.max(jnp.abs(delta))
    small = worst < 2.0**-8

    @pl.when(small)
    def _():
        y_ref[...] = near_identity(delta, row > lane, eye)

    @pl.when(jnp.logical_not(small))
    def _():
        y_ref[...] = eliminate(high + low) - eye.astype(F32)

    y = y_ref[...]
    rest = dot_full(y, exact)
    high, low = two_sum(exact, rest)
    unit = inverse_row * scale
    high_ref[...] = high * unit
    low_ref[...] = low * unit
    upper = product + dot_full(y, product)
    upper_ref[...] = jnp.where(row <= lane, upper, 0.0) * (size_row * (1.0 / scale))


def factor(gram, scale):
    k = gram.shape[0]
    return pl.pallas_call(
        lambda *refs: factor_kernel(scale, *refs),
        out_shape=(in_vmem(k, k), in_vmem(k, k), jax.ShapeDtypeStruct((k, k), F32)),
        in_specs=[VMEM_SPEC],
        out_specs=(VMEM_SPEC, VMEM_SPEC, VMEM_SPEC),
        scratch_shapes=[pltpu.VMEM((k, k), F32)],
        compiler_params=SMALL,
        name="factor",
    )(vmem(gram))


def basis_kernel(w_ref, high_ref, low_ref, out_ref):
    p1, p2, p3 = split3(high_ref[...])
    p4 = low_ref[...].astype(BF16)
    left = jnp.concatenate([p1, p1, p1, p2, p2, p3, p4], axis=1)
    for x in range(w_ref.shape[0]):
        w1, w2, w3 = split3(w_ref[x])
        right = jnp.concatenate([w3, w2, w1, w2, w1, w1, w1], axis=0)
        out_ref[:, x, :] = dot(left, right)


def basis_of(w, high, low):
    nx, k, plane = w.shape
    return pl.pallas_call(
        basis_kernel,
        out_shape=jax.ShapeDtypeStruct((k, nx, plane), F32),
        in_specs=[VMEM_SPEC] * 3,
        out_specs=VMEM_SPEC,
        compiler_params=SMALL,
        name="basis",
    )(vmem(w), vmem(high), vmem(low))


def per_device(vectors, reaction):
    k, nx, plane = vectors.shape
    peers = lax.axis_size(SFC_SUB)
    me = lax.axis_index(SFC_SUB)
    flags = jnp.stack([me % 2, (me > 0).astype(me.dtype), (me < peers - 1).astype(me.dtype)])
    inner, outer = borders(flags, vectors, reaction)
    across = [(i, i + 1) for i in range(1, peers - 1, 2)]
    within = [(i, i + 1) for i in range(0, peers, 2)]
    outer = lax.ppermute(outer, SFC_SUB, across + [(b, a) for a, b in across])
    inner = lax.ppermute(inner, SFC_SUB, within + [(b, a) for a, b in within])
    table = jnp.asarray(tables())
    field, both = begin(vectors, table)
    w, gram = operator_and_gram(flags, reaction, inner, outer, table, field, both)
    gram = sum_over_devices(gram)
    high, low, upper = factor(gram, math.sqrt(peers * nx * plane))
    return basis_of(w, high, low), upper


def solution(mesh):
    torus = Mesh(mesh.devices.reshape(16, 8, 4, 2), ("sfc_0", "sfc_1", "sub_0", "sub_1"))
    in_specs = (P(None, SFC_SUB, None), P(SFC_SUB, None))
    out_specs = (P(None, SFC_SUB, None), P())
    return jax.shard_map(
        per_device, mesh=torus, in_specs=in_specs, out_specs=out_specs, check_vma=False
    )
```

```python
import math

import jax
import jax.numpy as jnp
import numpy as np
from jax import lax
from jax.experimental import pallas as pl
from jax.experimental.pallas import tpu as pltpu
from jax.sharding import Mesh
from jax.sharding import PartitionSpec as P

NY = 32
NL = 8
PLANE = NY * NL
POWERS = 3
SFC_SUB = ("sfc_0", "sfc_1", "sub_0", "sub_1")
FAR = ("sfc_0",)
NEAR = ("sfc_1", "sub_0", "sub_1")
DELTA_MASS = 0.5
F32 = jnp.float32
BF16 = jnp.bfloat16


SMALL = pltpu.CompilerParams(vmem_limit_bytes=24 * 2**20)
VMEM_SPEC = pl.BlockSpec(memory_space=pltpu.VMEM)


def in_vmem(*shape):
    return pltpu.VMEM(shape, F32)


def vmem(array):
    return pltpu.with_memory_space_constraint(array, pltpu.VMEM)


def hbm(array):
    return pltpu.with_memory_space_constraint(array, pltpu.HBM)


def line_tables(count):
    index = np.arange(count)
    offset = index[:, None] - index[None, :]
    near = (np.abs(offset) == 1).astype(np.float32)
    same = (offset == 0).astype(np.float32)
    return 4.0 * same + near, 2.0 * same - near


def tables():
    mass_across, stiff_across = line_tables(NY)
    mass_layers, stiff_layers = line_tables(NL)
    mass = np.kron(mass_layers, mass_across)
    stiff = (
        6.0 * (np.kron(mass_layers, stiff_across) + np.kron(stiff_layers, mass_across))
        + DELTA_MASS * mass
    )
    return np.concatenate([stiff - 6.0 * mass, 4.0 * stiff + 12.0 * mass], axis=1).astype(BF16)


def split3(value):
    one = value.astype(BF16)
    rest = value - one.astype(F32)
    two = rest.astype(BF16)
    three = (rest - two.astype(F32)).astype(BF16)
    return one, two, three


def dot(a, b):
    return lax.dot_general(a, b, (((1,), (0,)), ((), ())), preferred_element_type=F32)


def dot_t(a, b):
    return lax.dot_general(a, b, (((1,), (1,)), ((), ())), preferred_element_type=F32)


def two_sum(a, b):
    s = a + b
    t = s - a
    return s, (a - (s - t)) + (b - t)


def power_below(x, square=False):
    low = -60 if square else -120
    p = jnp.full_like(x, 2.0**low)
    q = jnp.full_like(x, 2.0**-low)
    for k in (64, 32, 16, 8, 4, 2, 1) if square else (128, 64, 32, 16, 8, 4, 2, 1):
        half = 2.0 ** (k // 2) if k > 1 else 2.0
        up = p * half * (half if k > 1 else 1.0)
        down = q * (1.0 / half) * (1.0 / half if k > 1 else 1.0)
        fits = (up * up if square else up) <= x
        p, q = jnp.where(fits, up, p), jnp.where(fits, down, q)
    return p, q


def digits(value, count, extra=None, extra_at=3):
    out = []
    rest = value
    for i in range(count):
        digit = jnp.round(rest)
        out.append(digit.astype(BF16))
        rest = rest - digit
        if extra is not None and i == extra_at - 1:
            rest = rest + extra * (256.0 ** (extra_at - 1))
        rest = rest * 256.0
    return out


def levels_to_pair(levels):
    high = levels[-1]
    low = jnp.zeros_like(high)
    for level in reversed(levels[:-1]):
        high, err = two_sum(level, high * (1.0 / 256.0))
        low = low * (1.0 / 256.0) + err
    return high, low


def border_kernel(odd_ref, vec_ref, react_ref, table_ref, inner_ref, outer_ref, own_ref, own_react_ref, own_table_ref, sems):
    k, nx, plane = vec_ref.shape
    parts = 4
    copies = []
    for part in range(parts):
        rows = pl.ds(part * (k // parts), k // parts)
        copies.append(pltpu.make_async_copy(vec_ref.at[rows], own_ref.at[rows], sems.at[part]))
    copies.append(pltpu.make_async_copy(react_ref, own_react_ref, sems.at[parts]))
    copies.append(pltpu.make_async_copy(table_ref, own_table_ref, sems.at[parts + 1]))
    for copy in copies:
        copy.start()
    copies[-2].wait()
    odd = odd_ref[0]

    def fill(ref, start, rows):
        for j in range(POWERS):
            ref[j, rows, :] = own_ref[rows, start + j, :]
            if rows.start == 0:
                ref[j, k:, :] = jnp.broadcast_to(own_react_ref[start + j : start + j + 1, :], (8, plane))

    for part in range(parts):
        rows = pl.ds(part * (k // parts), k // parts)
        copies[part].wait()

        @pl.when(odd == 0)
        def _():
            fill(inner_ref, nx - POWERS, rows)
            fill(outer_ref, 0, rows)

        @pl.when(odd != 0)
        def _():
            fill(inner_ref, 0, rows)
            fill(outer_ref, nx - POWERS, rows)

    copies[-1].wait()


def borders(odd, vectors, reaction, table):
    k, _, plane = vectors.shape
    shape = in_vmem(POWERS, k + 8, plane)
    anywhere = pl.BlockSpec(memory_space=pltpu.HBM)
    return pl.pallas_call(
        border_kernel,
        out_shape=(shape, shape, in_vmem(*vectors.shape), in_vmem(*reaction.shape), pltpu.VMEM(table.shape, table.dtype)),
        in_specs=[pl.BlockSpec(memory_space=pltpu.SMEM), anywhere, anywhere, anywhere],
        out_specs=(VMEM_SPEC,) * 5,
        scratch_shapes=[pltpu.SemaphoreType.DMA((6,))],
        compiler_params=SMALL,
        name="borders",
    )(odd, hbm(vectors), hbm(reaction), hbm(table))


def products(field, both, table, start, count):
    k = field.shape[1]
    n = count * k
    one, two, three = split3(field[pl.ds(start, count)].reshape(n, PLANE))
    parts = dot(jnp.concatenate([one, two, three], axis=0), table)
    both[pl.ds(start, count)] = (parts[:n] + parts[n : 2 * n] + parts[2 * n :]).reshape(count, k, 2 * PLANE)


def begin_kernel(vec_ref, table_ref, field, both):
    _, nx, _ = vec_ref.shape
    for x in range(nx):
        field[x] = vec_ref[:, x, :]
    table = table_ref[...]

    def one_part(i, _):
        products(field, both, table, 0, nx)
        return 0

    lax.fori_loop(0, 1, one_part, 0)


def begin(vectors, table):
    k, nx, plane = vectors.shape
    return pl.pallas_call(
        begin_kernel,
        out_shape=(in_vmem(nx, k, plane), in_vmem(nx, k, 2 * plane)),
        in_specs=[VMEM_SPEC, VMEM_SPEC],
        out_specs=(VMEM_SPEC, VMEM_SPEC),
        cost_estimate=pl.CostEstimate(flops=2 * 3 * nx * k * plane * 2 * plane, bytes_accessed=0, transcendentals=0),
        compiler_params=SMALL,
        name="begin",
    )(vmem(vectors), vmem(table))


def operator_kernel(k, nx, flags_ref, react_ref, inner_ref, outer_ref, table_ref, own_ref, own_both_ref, w_ref, gram_ref, field, both, react):
    halo = POWERS
    total = nx + 2 * halo
    odd = flags_ref[0]
    low_inside = flags_ref[1].astype(F32)
    high_inside = flags_ref[2].astype(F32)
    react[halo : halo + nx] = react_ref[...]

    def fill(low_ref, high_ref):
        field[0:halo] = low_ref[:, :k, :]
        field[halo + nx : total] = high_ref[:, :k, :]
        react[0:halo] = low_ref[:, k, :]
        react[halo + nx : total] = high_ref[:, k, :]

    @pl.when(odd == 0)
    def _():
        fill(outer_ref, inner_ref)

    @pl.when(odd != 0)
    def _():
        fill(inner_ref, outer_ref)

    table = table_ref[...]

    def combine(step, x, values, parts, offset):
        value = (
            parts[x - 1 - offset, :, :PLANE] + parts[x + 1 - offset, :, :PLANE] + parts[x - offset, :, PLANE:]
        ) * (1.0 / 216.0) + react[pl.ds(x, 1), :] * values[x - offset]
        if step < POWERS - 1:
            keep = jnp.where(x < halo, low_inside, jnp.where(x >= halo + nx, high_inside, 1.0))
            field[x] = value * keep
        else:
            w_ref[x - halo] = value
        return 0

    def edge(i, _):
        products(field, both, table, i * (halo + nx), halo)
        return 0

    lax.fori_loop(0, 2, edge, 0)

    def own_edge(i, _):
        x = jnp.where(i < 2, i, nx - 4 + i)
        field[halo + x] = own_ref[x]
        both[halo + x] = own_both_ref[x]
        return 0

    lax.fori_loop(0, 4, own_edge, 0)

    def outside(i, _):
        x = jnp.where(i < halo, 1 + i, nx - 1 + i)
        return combine(0, x, field, both, 0)

    lax.fori_loop(0, 2 * halo, outside, 0)

    def inside(x, _):
        return combine(0, x, own_ref, own_both_ref, halo)

    lax.fori_loop(halo + 1, halo + nx - 1, inside, 0, unroll=7)
    for step in range(1, POWERS):
        first, last = step, total - step

        def product(i, _):
            products(field, both, table, first, last - first)
            return 0

        lax.fori_loop(0, 1, product, 0)

        def later(x, _):
            return combine(step, x, field, both, 0)

        lax.fori_loop(first + 1, last - 1, later, 0, unroll=(last - first - 2) // 2)
    peak = jnp.abs(w_ref[0])
    for x in range(1, nx):
        peak = jnp.maximum(peak, jnp.abs(w_ref[x]))
    peak = jnp.max(peak, axis=1, keepdims=True)
    size, inverse = power_below(peak)
    scale = inverse * 64.0
    slices = 4
    group = 4
    pairs = None
    for start in range(0, nx, group):
        parts = [[] for _ in range(slices)]
        for x in range(start, start + group):
            for s, digit in enumerate(digits(w_ref[x] * scale, slices)):
                parts[s].append(digit)
        stack = jnp.concatenate([jnp.concatenate(p, axis=1) for p in parts], axis=0)
        counts = dot_t(stack, stack)
        block = [[counts[i * k : (i + 1) * k, j * k : (j + 1) * k] for j in range(slices)] for i in range(slices)]
        tail = [
            sum(block[i][level - i] for i in range(slices) if 0 <= level - i < slices)
            for level in range(3, 2 * slices - 1)
        ]
        rest = tail[-1]
        for value in reversed(tail[:-1]):
            rest = value + rest * (1.0 / 256.0)
        terms = [
            rest * 2.0**-24,
            block[1][1] * 2.0**-16,
            (block[0][2] + block[2][0]) * 2.0**-16,
            block[0][1] * 2.0**-8,
            block[1][0] * 2.0**-8,
            block[0][0],
        ]
        for term in terms:
            if pairs is None:
                pairs = (term, jnp.zeros_like(term))
            else:
                high, err = two_sum(pairs[0], term)
                pairs = (high, pairs[1] + err)
    high, err = two_sum(pairs[0], pairs[1])
    row = size * (1.0 / 64.0)
    eye = lax.broadcasted_iota(jnp.int32, (k, k), 0) == lax.broadcasted_iota(jnp.int32, (k, k), 1)
    column = jnp.sum(jnp.where(eye, row, 0.0), axis=0, keepdims=True)
    gram_ref[:, 0, :] = jnp.concatenate([high * row * column, err * row * column], axis=1)


def operator_and_gram(flags, reaction, inner, outer, table, own, own_both):
    nx, k, plane = own.shape
    total = nx + 2 * POWERS
    smem = pl.BlockSpec(memory_space=pltpu.SMEM)
    return pl.pallas_call(
        lambda *refs: operator_kernel(k, nx, *refs),
        out_shape=(in_vmem(nx, k, plane), in_vmem(k, 1, 2 * k)),
        in_specs=[smem] + [VMEM_SPEC] * 6,
        out_specs=(VMEM_SPEC, VMEM_SPEC),
        scratch_shapes=[
            pltpu.VMEM((total, k, plane), F32),
            pltpu.VMEM((total, k, 2 * plane), F32),
            pltpu.VMEM((total, plane), F32),
        ],
        cost_estimate=pl.CostEstimate(flops=2 * 3 * 44 * k * plane * 2 * plane, bytes_accessed=0, transcendentals=0),
        compiler_params=SMALL,
        name="operator_gram",
    )(flags, vmem(reaction), vmem(inner), vmem(outer), vmem(table), vmem(own), vmem(own_both))


def pair_sum_kernel(parts_ref, out_ref):
    value = parts_ref[:, 0, :]
    width = value.shape[1]
    half = width // 2
    error = jnp.zeros_like(value)
    while value.shape[0] > 1:
        n = value.shape[0] // 2
        value, err = two_sum(value[:n], value[n:])
        error = error[:n] + error[n:] + err
    low = pltpu.roll(value, half, 1) + error
    high, err = two_sum(value, low)
    lane = lax.broadcasted_iota(jnp.int32, value.shape, 1)
    row = jnp.where(lane < half, high, pltpu.roll(err, half, 1))
    out_ref[:, 0, :] = jnp.broadcast_to(row, (out_ref.shape[0], width))


def pair_sum(parts, copies):
    return pl.pallas_call(
        pair_sum_kernel,
        out_shape=in_vmem(copies, 1, parts.shape[2]),
        in_specs=[VMEM_SPEC],
        out_specs=VMEM_SPEC,
        compiler_params=SMALL,
        name="pair_sum",
    )(vmem(parts))


def sum_over_devices(gram):
    near = lax.axis_size(NEAR)
    far = lax.axis_size(FAR)
    rows = lax.all_to_all(gram, NEAR, 0, 0)
    mine = pair_sum(rows, far)
    mine = pair_sum(lax.all_to_all(mine, FAR, 0, 0), near)
    return lax.all_to_all(mine, NEAR, 0, 0)


def level_sums(counts, k, rows, columns):
    out = []
    for level in range(rows + columns - 1):
        terms = [
            counts[i * k : (i + 1) * k, (level - i) * k : (level - i + 1) * k]
            for i in range(rows)
            if 0 <= level - i < columns
        ]
        total = terms[0]
        for term in terms[1:]:
            total = total + term
        out.append(total)
    return out


def dot_of_stack(a_parts, b_parts):
    return dot(jnp.concatenate(a_parts, axis=1), jnp.concatenate(b_parts, axis=0))


def dot_full(a, b):
    a1, a2, a3 = split3(a)
    b1, b2, b3 = split3(b)
    return dot_of_stack([a1, a1, a2, a1, a2, a3], [b1, b2, b1, b3, b2, b1])


def eliminate(square):
    k = square.shape[0]
    row = lax.broadcasted_iota(jnp.int32, (k, k), 0)
    lane = lax.broadcasted_iota(jnp.int32, (k, k), 1)
    eye = (row == lane).astype(F32)
    block = 8
    work = jnp.concatenate([square, eye], axis=1)
    done = []
    for start in range(0, k, block):
        rows = work.shape[0]
        columns = [jnp.broadcast_to(work[:, start + a : start + a + 1], (rows, 2 * k)) for a in range(block)]
        below = lax.broadcasted_iota(jnp.int32, (rows, 2 * k), 0)
        for a in range(0, block, 2):
            one, two = columns[a], columns[a + 1]
            p, q, r = one[a : a + 1, :], two[a : a + 1, :], two[a + 1 : a + 2, :]
            inverse = 1.0 / (p * r - q * q)
            first = jnp.where(below > a + 1, (one * r - two * q) * inverse, 0.0)
            second = jnp.where(below > a + 1, (two * p - one * q) * inverse, 0.0)
            for b in range(a + 2, block):
                columns[b] = columns[b] - (first * columns[b][a : a + 1, :] + second * columns[b][a + 1 : a + 2, :])
            work = work - (first * work[a : a + 1, :] + second * work[a + 1 : a + 2, :])
        done.append(work[:block])
        work = work[block:]
    work = jnp.concatenate(done, axis=0)
    pivot = jnp.sum(work[:, :k] * eye, axis=1, keepdims=True)
    beside = jnp.sum(jnp.where((row == lane + 1) & (row % 2 == 1), work[:, :k], 0.0), axis=1, keepdims=True)
    ratio = beside / pltpu.roll(jnp.broadcast_to(pivot, (k, 2 * k)), 1, 0)
    work = work - ratio * pltpu.roll(work, 1, 0)
    pivot = pivot - ratio[:, :k] * beside
    return work[:, k:] * lax.rsqrt(pivot)


def near_identity(delta, strict, half):
    def lower(value):
        return jnp.where(strict, value, jnp.where(half, 0.5 * value, 0.0))

    def pair(value):
        one = value.astype(BF16)
        return one, (value - one.astype(F32)).astype(BF16)

    d1, d2 = pair(delta)
    right = jnp.concatenate([d1, d2, d1], axis=0)
    y = -lower(delta)
    for _ in range(2):
        y1, y2 = pair(y)
        outer = y + dot(jnp.concatenate([y1, y1, y2], axis=1), right)
        o1, o2 = pair(outer)
        square = dot_t(jnp.concatenate([o1, o1, o2], axis=1), jnp.concatenate([y1, y2, y1], axis=1))
        error = lower(delta + outer + outer.T + square)
        e1, e2 = pair(error)
        y = y - error - dot_of_stack([e1, e1, e2], [y1, y2, y1])
    return y


def factor_kernel(scale, gram_ref, high_ref, low_ref, upper_ref, y_ref):
    k = gram_ref.shape[0]
    pair = gram_ref[:, 0, :]
    high, low = pair[:, :k], pair[:, k:]
    row = lax.broadcasted_iota(jnp.int32, (k, k), 0)
    lane = lax.broadcasted_iota(jnp.int32, (k, k), 1)
    eye = row == lane
    diagonal = jnp.where(eye, high, 0.0)
    size_row, inverse_row = power_below(jnp.sum(diagonal, axis=0, keepdims=True), square=True)
    _, inverse_column = power_below(jnp.sum(diagonal, axis=1, keepdims=True), square=True)
    unit = inverse_column * inverse_row
    high = high * unit
    low = low * unit
    gram_digits = digits(high * 32.0, 6, extra=low * 32.0)
    guess = eliminate(high)
    top, top_inverse = power_below(jnp.max(jnp.abs(guess), axis=1, keepdims=True))
    guess_digits = digits(guess * top_inverse * 64.0, 3)
    exact = sum(d.astype(F32) * 256.0**-i for i, d in enumerate(guess_digits))
    exact = exact * (top * (1.0 / 64.0))
    guess_stack = jnp.concatenate(guess_digits, axis=0)
    counts = dot(guess_stack, jnp.concatenate(gram_digits, axis=1))
    high, low = levels_to_pair(level_sums(counts, k, 3, 6))
    product = (high + low) * (top * 2.0**-11)
    big, big_inverse = power_below(jnp.max(jnp.abs(high), axis=1, keepdims=True))
    product_digits = digits(high * big_inverse * 64.0, 6, extra=low * big_inverse * 64.0)
    counts = dot_t(jnp.concatenate(product_digits, axis=0), guess_stack)
    high, low = levels_to_pair(level_sums(counts, k, 6, 3))
    top_row = jnp.sum(jnp.where(eye, top, 0.0), axis=0, keepdims=True)
    unit = (top * 2.0**-11) * (big * (1.0 / 64.0)) * (top_row * (1.0 / 64.0))
    high = high * unit
    low = low * unit
    delta = jnp.where(eye, high - 1.0, high) + low
    worst = jnp.max(jnp.abs(delta))
    small = worst < 2.0**-9

    @pl.when(small)
    def _():
        y_ref[...] = near_identity(delta, row > lane, eye)

    @pl.when(jnp.logical_not(small))
    def _():
        y_ref[...] = eliminate(high + low) - eye.astype(F32)

    y = y_ref[...]
    rest = dot_full(y, exact)
    high, low = two_sum(exact, rest)
    unit = inverse_row * scale
    high_ref[...] = high * unit
    low_ref[...] = low * unit
    upper = product + dot_full(y, product)
    upper_ref[...] = jnp.where(row <= lane, upper, 0.0) * (size_row * (1.0 / scale))


def factor(gram, scale):
    k = gram.shape[0]
    return pl.pallas_call(
        lambda *refs: factor_kernel(scale, *refs),
        out_shape=(in_vmem(k, k), in_vmem(k, k), jax.ShapeDtypeStruct((k, k), F32)),
        in_specs=[VMEM_SPEC],
        out_specs=(VMEM_SPEC, VMEM_SPEC, VMEM_SPEC),
        scratch_shapes=[pltpu.VMEM((k, k), F32)],
        compiler_params=SMALL,
        name="factor",
    )(vmem(gram))


def basis_kernel(w_ref, high_ref, low_ref, out_ref, result, sems):
    _, nx, _ = result.shape
    p1, p2, p3 = split3(high_ref[...])
    p4 = low_ref[...].astype(BF16)
    left = jnp.concatenate([p1, p1, p1, p2, p2, p3, p4], axis=1)
    copies = []
    for x in range(nx):
        w1, w2, w3 = split3(w_ref[x])
        right = jnp.concatenate([w3, w2, w1, w2, w1, w1, w1], axis=0)
        result[:, x, :] = dot(left, right)
        if (x + 1) % 8 == 0:
            rows = pl.ds(x - 7, 8)
            copies.append(pltpu.make_async_copy(result.at[:, rows, :], out_ref.at[:, rows, :], sems.at[x // 8]))
            copies[-1].start()
    for copy in copies:
        copy.wait()


def basis_of(w, high, low):
    nx, k, plane = w.shape
    return pl.pallas_call(
        basis_kernel,
        out_shape=jax.ShapeDtypeStruct((k, nx, plane), F32),
        in_specs=[VMEM_SPEC] * 3,
        out_specs=pl.BlockSpec(memory_space=pltpu.HBM),
        scratch_shapes=[pltpu.VMEM((k, nx, plane), F32), pltpu.SemaphoreType.DMA((nx // 8,))],
        compiler_params=SMALL,
        name="basis",
    )(vmem(w), vmem(high), vmem(low))


def device_program(vectors, reaction):
    _, nx, plane = vectors.shape
    peers = lax.axis_size(SFC_SUB)
    me = lax.axis_index(SFC_SUB)
    flags = jnp.stack([me % 2, (me > 0).astype(me.dtype), (me < peers - 1).astype(me.dtype)])
    inner, outer, vectors, reaction, table = borders(flags, vectors, reaction, jnp.asarray(tables()))
    across = [(i, i + 1) for i in range(1, peers - 1, 2)]
    within = [(i, i + 1) for i in range(0, peers, 2)]
    outer = lax.ppermute(outer, SFC_SUB, across + [(b, a) for a, b in across])
    inner = lax.ppermute(inner, SFC_SUB, within + [(b, a) for a, b in within])
    field, both = begin(vectors, table)
    w, gram = operator_and_gram(flags, reaction, inner, outer, table, field, both)
    gram = sum_over_devices(gram)
    high, low, upper = factor(gram, math.sqrt(peers * nx * plane))
    return basis_of(w, high, low), upper


def solution(mesh):
    torus = Mesh(mesh.devices.reshape(16, 8, 4, 2), ("sfc_0", "sfc_1", "sub_0", "sub_1"))
    in_specs = (P(None, SFC_SUB, None), P(SFC_SUB, None))
    out_specs = (P(None, SFC_SUB, None), P())
    return jax.shard_map(device_program, mesh=torus, in_specs=in_specs, out_specs=out_specs, check_vma=False)
```

```python
import math

import jax
import jax.numpy as jnp
import numpy as np
from jax import lax
from jax.experimental import pallas as pl
from jax.experimental.pallas import tpu as pltpu
from jax.sharding import Mesh
from jax.sharding import PartitionSpec as P

NY = 32
NL = 8
PLANE = NY * NL
POWERS = 3
SFC_SUB = ("sfc_0", "sfc_1", "sub_0", "sub_1")
FAR = ("sfc_0",)
NEAR = ("sfc_1", "sub_0", "sub_1")
DELTA_MASS = 0.5
F32 = jnp.float32
BF16 = jnp.bfloat16


SMALL = pltpu.CompilerParams(vmem_limit_bytes=24 * 2**20)
VMEM_SPEC = pl.BlockSpec(memory_space=pltpu.VMEM)


def in_vmem(*shape):
    return pltpu.VMEM(shape, F32)


def vmem(array):
    return pltpu.with_memory_space_constraint(array, pltpu.VMEM)


def hbm(array):
    return pltpu.with_memory_space_constraint(array, pltpu.HBM)


def line_tables(count):
    index = np.arange(count)
    offset = index[:, None] - index[None, :]
    near = (np.abs(offset) == 1).astype(np.float32)
    same = (offset == 0).astype(np.float32)
    return 4.0 * same + near, 2.0 * same - near


def tables():
    mass_across, stiff_across = line_tables(NY)
    mass_layers, stiff_layers = line_tables(NL)
    mass = np.kron(mass_layers, mass_across)
    stiff = (
        6.0 * (np.kron(mass_layers, stiff_across) + np.kron(stiff_layers, mass_across))
        + DELTA_MASS * mass
    )
    return np.concatenate([stiff - 6.0 * mass, 4.0 * stiff + 12.0 * mass], axis=1).astype(BF16)


def split3(value):
    one = value.astype(BF16)
    rest = value - one.astype(F32)
    two = rest.astype(BF16)
    three = (rest - two.astype(F32)).astype(BF16)
    return one, two, three


def dot(a, b):
    return lax.dot_general(a, b, (((1,), (0,)), ((), ())), preferred_element_type=F32)


def dot_t(a, b):
    return lax.dot_general(a, b, (((1,), (1,)), ((), ())), preferred_element_type=F32)


def two_sum(a, b):
    s = a + b
    t = s - a
    return s, (a - (s - t)) + (b - t)


def power_below(x, square=False):
    low = -60 if square else -120
    p = jnp.full_like(x, 2.0**low)
    q = jnp.full_like(x, 2.0**-low)
    for k in (64, 32, 16, 8, 4, 2, 1) if square else (128, 64, 32, 16, 8, 4, 2, 1):
        half = 2.0 ** (k // 2) if k > 1 else 2.0
        up = p * half * (half if k > 1 else 1.0)
        down = q * (1.0 / half) * (1.0 / half if k > 1 else 1.0)
        fits = (up * up if square else up) <= x
        p, q = jnp.where(fits, up, p), jnp.where(fits, down, q)
    return p, q


def digits(value, count, extra=None, extra_at=3):
    out = []
    rest = value
    for i in range(count):
        digit = jnp.round(rest)
        out.append(digit.astype(BF16))
        rest = rest - digit
        if extra is not None and i == extra_at - 1:
            rest = rest + extra * (256.0 ** (extra_at - 1))
        rest = rest * 256.0
    return out


def levels_to_pair(levels):
    high = levels[-1]
    low = jnp.zeros_like(high)
    for level in reversed(levels[:-1]):
        high, err = two_sum(level, high * (1.0 / 256.0))
        low = low * (1.0 / 256.0) + err
    return high, low


def border_kernel(odd_ref, vec_ref, react_ref, table_ref, inner_ref, outer_ref, own_ref, own_react_ref, own_table_ref, sems):
    k, nx, plane = vec_ref.shape
    parts = 4
    copies = []
    for part in range(parts):
        rows = pl.ds(part * (k // parts), k // parts)
        copies.append(pltpu.make_async_copy(vec_ref.at[rows], own_ref.at[rows], sems.at[part]))
    copies.append(pltpu.make_async_copy(react_ref, own_react_ref, sems.at[parts]))
    copies.append(pltpu.make_async_copy(table_ref, own_table_ref, sems.at[parts + 1]))
    for copy in copies:
        copy.start()
    copies[-2].wait()
    odd = odd_ref[0]

    def fill(ref, start, rows):
        for j in range(POWERS):
            ref[j, rows, :] = own_ref[rows, start + j, :]
            if rows.start == 0:
                ref[j, k:, :] = jnp.broadcast_to(own_react_ref[start + j : start + j + 1, :], (8, plane))

    for part in range(parts):
        rows = pl.ds(part * (k // parts), k // parts)
        copies[part].wait()

        @pl.when(odd == 0)
        def _():
            fill(inner_ref, nx - POWERS, rows)
            fill(outer_ref, 0, rows)

        @pl.when(odd != 0)
        def _():
            fill(inner_ref, 0, rows)
            fill(outer_ref, nx - POWERS, rows)

    copies[-1].wait()


def borders(odd, vectors, reaction, table):
    k, _, plane = vectors.shape
    shape = in_vmem(POWERS, k + 8, plane)
    anywhere = pl.BlockSpec(memory_space=pltpu.HBM)
    return pl.pallas_call(
        border_kernel,
        out_shape=(shape, shape, in_vmem(*vectors.shape), in_vmem(*reaction.shape), pltpu.VMEM(table.shape, table.dtype)),
        in_specs=[pl.BlockSpec(memory_space=pltpu.SMEM), anywhere, anywhere, anywhere],
        out_specs=(VMEM_SPEC,) * 5,
        scratch_shapes=[pltpu.SemaphoreType.DMA((6,))],
        compiler_params=SMALL,
        name="borders",
    )(odd, hbm(vectors), hbm(reaction), hbm(table))


def products(field, both, table, start, count):
    k = field.shape[1]
    n = count * k
    one, two, three = split3(field[pl.ds(start, count)].reshape(n, PLANE))
    parts = dot(jnp.concatenate([one, two, three], axis=0), table)
    both[pl.ds(start, count)] = (parts[:n] + parts[n : 2 * n] + parts[2 * n :]).reshape(count, k, 2 * PLANE)


def begin_kernel(vec_ref, react_ref, table_ref, own, own_both, first, first_both):
    _, nx, _ = vec_ref.shape
    for x in range(nx):
        own[x] = vec_ref[:, x, :]
    table = table_ref[...]

    def own_products(i, _):
        products(own, own_both, table, 0, nx)
        return 0

    lax.fori_loop(0, 1, own_products, 0)

    def inside(x, _):
        first[x - 1] = combination(own_both, own, react_ref, x, x)
        return 0

    lax.fori_loop(1, nx - 1, inside, 0, unroll=7)

    def first_products(i, _):
        products(first, first_both, table, 0, nx - 2)
        return 0

    lax.fori_loop(0, 1, first_products, 0)


def combination(both, field, react, x, at):
    return (both[x - 1, :, :PLANE] + both[x + 1, :, :PLANE] + both[x, :, PLANE:]) * (1.0 / 216.0) + react[
        pl.ds(at, 1), :
    ] * field[x]


def begin(vectors, reaction, table):
    k, nx, plane = vectors.shape
    return pl.pallas_call(
        begin_kernel,
        out_shape=(
            in_vmem(nx, k, plane),
            in_vmem(nx, k, 2 * plane),
            in_vmem(nx - 2, k, plane),
            in_vmem(nx - 2, k, 2 * plane),
        ),
        in_specs=[VMEM_SPEC] * 3,
        out_specs=(VMEM_SPEC,) * 4,
        cost_estimate=pl.CostEstimate(flops=12 * (nx + nx - 2) * k * plane * plane, bytes_accessed=0, transcendentals=0),
        compiler_params=SMALL,
        name="begin",
    )(vmem(vectors), vmem(reaction), vmem(table))


def operator_kernel(k, nx, flags_ref, react_ref, inner_ref, outer_ref, table_ref, own, own_both, first, first_both, w_ref, gram_ref, field, both, react):
    halo = POWERS
    total = nx + 2 * halo
    top = halo + nx
    odd = flags_ref[0]
    low_inside = flags_ref[1].astype(F32)
    high_inside = flags_ref[2].astype(F32)
    react[halo:top] = react_ref[...]

    def fill(low_ref, high_ref):
        field[0:halo] = low_ref[:, :k, :]
        field[top:total] = high_ref[:, :k, :]
        react[0:halo] = low_ref[:, k, :]
        react[top:total] = high_ref[:, k, :]

    @pl.when(odd == 0)
    def _():
        fill(outer_ref, inner_ref)

    @pl.when(odd != 0)
    def _():
        fill(inner_ref, outer_ref)

    table = table_ref[...]

    def keep(x):
        return jnp.where(x < halo, low_inside, jnp.where(x >= top, high_inside, 1.0))

    def step(x, _):
        field[x] = combination(both, field, react, x, x) * keep(x)
        return 0

    def ends(body, low, high, count):
        lax.fori_loop(0, 2 * count, lambda i, c: body(jnp.where(i < count, low + i, high + i - count), c), 0, unroll=count)

    def border_products(i, _):
        products(field, both, table, i * top, halo)
        return 0

    lax.fori_loop(0, 2, border_products, 0)

    def own_edge(x, _):
        field[x] = own[x - halo]
        both[x] = own_both[x - halo]
        return 0

    ends(own_edge, halo, top - 2, 2)
    ends(step, 1, top - 1, 3)

    def edge_products(i, _):
        products(field, both, table, 1 + i * (top - 2), halo)
        return 0

    lax.fori_loop(0, 2, edge_products, 0)

    def first_edge(x, _):
        field[x] = first[x - halo - 1]
        both[x] = first_both[x - halo - 1]
        return 0

    ends(first_edge, halo + 1, top - 3, 2)
    ends(step, 2, top - 2, 3)

    def inside(x, _):
        field[x] = combination(first_both, first, react, x - halo - 1, x)
        return 0

    lax.fori_loop(halo + 2, top - 2, inside, 0, unroll=6)

    def third_products(i, _):
        products(field, both, table, 2, total - 4)
        return 0

    lax.fori_loop(0, 1, third_products, 0)

    def last(x, _):
        w_ref[x - halo] = combination(both, field, react, x, x)
        return 0

    lax.fori_loop(halo, top, last, 0, unroll=8)
    peak = jnp.abs(w_ref[0])
    for x in range(1, nx):
        peak = jnp.maximum(peak, jnp.abs(w_ref[x]))
    peak = jnp.max(peak, axis=1, keepdims=True)
    size, inverse = power_below(peak)
    scale = inverse * 64.0
    slices = 4
    group = 4
    pairs = None
    for start in range(0, nx, group):
        parts = [[] for _ in range(slices)]
        for x in range(start, start + group):
            for s, digit in enumerate(digits(w_ref[x] * scale, slices)):
                parts[s].append(digit)
        stack = jnp.concatenate([jnp.concatenate(p, axis=1) for p in parts], axis=0)
        counts = dot_t(stack, stack)
        block = [[counts[i * k : (i + 1) * k, j * k : (j + 1) * k] for j in range(slices)] for i in range(slices)]
        tail = [
            sum(block[i][level - i] for i in range(slices) if 0 <= level - i < slices)
            for level in range(3, 2 * slices - 1)
        ]
        rest = tail[-1]
        for value in reversed(tail[:-1]):
            rest = value + rest * (1.0 / 256.0)
        terms = [
            rest * 2.0**-24,
            block[1][1] * 2.0**-16,
            (block[0][2] + block[2][0]) * 2.0**-16,
            block[0][1] * 2.0**-8,
            block[1][0] * 2.0**-8,
            block[0][0],
        ]
        for term in terms:
            if pairs is None:
                pairs = (term, jnp.zeros_like(term))
            else:
                high, err = two_sum(pairs[0], term)
                pairs = (high, pairs[1] + err)
    high, err = two_sum(pairs[0], pairs[1])
    row = size * (1.0 / 64.0)
    eye = lax.broadcasted_iota(jnp.int32, (k, k), 0) == lax.broadcasted_iota(jnp.int32, (k, k), 1)
    column = jnp.sum(jnp.where(eye, row, 0.0), axis=0, keepdims=True)
    gram_ref[:, 0, :] = jnp.concatenate([high * row * column, err * row * column], axis=1)


def operator_and_gram(flags, reaction, inner, outer, table, begun):
    nx, k, plane = begun[0].shape
    total = nx + 2 * POWERS
    smem = pl.BlockSpec(memory_space=pltpu.SMEM)
    return pl.pallas_call(
        lambda *refs: operator_kernel(k, nx, *refs),
        out_shape=(in_vmem(nx, k, plane), in_vmem(k, 1, 2 * k)),
        in_specs=[smem] + [VMEM_SPEC] * 8,
        out_specs=(VMEM_SPEC, VMEM_SPEC),
        scratch_shapes=[
            pltpu.VMEM((total, k, plane), F32),
            pltpu.VMEM((total, k, 2 * plane), F32),
            pltpu.VMEM((total + 18, plane), F32),
        ],
        cost_estimate=pl.CostEstimate(flops=2 * 3 * 30 * k * plane * 2 * plane, bytes_accessed=0, transcendentals=0),
        compiler_params=SMALL,
        name="operator_gram",
    )(flags, vmem(reaction), vmem(inner), vmem(outer), vmem(table), *map(vmem, begun))


def pair_sum_kernel(parts_ref, out_ref):
    value = parts_ref[:, 0, :]
    width = value.shape[1]
    half = width // 2
    error = jnp.zeros_like(value)
    while value.shape[0] > 1:
        n = value.shape[0] // 2
        value, err = two_sum(value[:n], value[n:])
        error = error[:n] + error[n:] + err
    low = pltpu.roll(value, half, 1) + error
    high, err = two_sum(value, low)
    lane = lax.broadcasted_iota(jnp.int32, value.shape, 1)
    row = jnp.where(lane < half, high, pltpu.roll(err, half, 1))
    out_ref[:, 0, :] = jnp.broadcast_to(row, (out_ref.shape[0], width))


def pair_sum(parts, copies):
    return pl.pallas_call(
        pair_sum_kernel,
        out_shape=in_vmem(copies, 1, parts.shape[2]),
        in_specs=[VMEM_SPEC],
        out_specs=VMEM_SPEC,
        compiler_params=SMALL,
        name="pair_sum",
    )(vmem(parts))


def sum_over_devices(gram):
    near = lax.axis_size(NEAR)
    far = lax.axis_size(FAR)
    rows = lax.all_to_all(gram, NEAR, 0, 0)
    mine = pair_sum(rows, far)
    mine = pair_sum(lax.all_to_all(mine, FAR, 0, 0), near)
    return lax.all_to_all(mine, NEAR, 0, 0)


def level_sums(counts, k, rows, columns):
    out = []
    for level in range(rows + columns - 1):
        terms = [
            counts[i * k : (i + 1) * k, (level - i) * k : (level - i + 1) * k]
            for i in range(rows)
            if 0 <= level - i < columns
        ]
        total = terms[0]
        for term in terms[1:]:
            total = total + term
        out.append(total)
    return out


def dot_of_stack(a_parts, b_parts):
    return dot(jnp.concatenate(a_parts, axis=1), jnp.concatenate(b_parts, axis=0))


def dot_full(a, b):
    a1, a2, a3 = split3(a)
    b1, b2, b3 = split3(b)
    return dot_of_stack([a1, a1, a2, a1, a2, a3], [b1, b2, b1, b3, b2, b1])


def eliminate(square):
    k = square.shape[0]
    row = lax.broadcasted_iota(jnp.int32, (k, k), 0)
    lane = lax.broadcasted_iota(jnp.int32, (k, k), 1)
    eye = (row == lane).astype(F32)
    block = 8
    work = jnp.concatenate([square, eye], axis=1)
    done = []
    for start in range(0, k, block):
        rows = work.shape[0]
        columns = [jnp.broadcast_to(work[:, start + a : start + a + 1], (rows, 2 * k)) for a in range(block)]
        below = lax.broadcasted_iota(jnp.int32, (rows, 2 * k), 0)
        for a in range(0, block, 2):
            one, two = columns[a], columns[a + 1]
            p, q, r = one[a : a + 1, :], two[a : a + 1, :], two[a + 1 : a + 2, :]
            inverse = 1.0 / (p * r - q * q)
            first = jnp.where(below > a + 1, (one * r - two * q) * inverse, 0.0)
            second = jnp.where(below > a + 1, (two * p - one * q) * inverse, 0.0)
            for b in range(a + 2, block):
                columns[b] = columns[b] - (first * columns[b][a : a + 1, :] + second * columns[b][a + 1 : a + 2, :])
            work = work - (first * work[a : a + 1, :] + second * work[a + 1 : a + 2, :])
        done.append(work[:block])
        work = work[block:]
    work = jnp.concatenate(done, axis=0)
    pivot = jnp.sum(work[:, :k] * eye, axis=1, keepdims=True)
    beside = jnp.sum(jnp.where((row == lane + 1) & (row % 2 == 1), work[:, :k], 0.0), axis=1, keepdims=True)
    ratio = beside / pltpu.roll(jnp.broadcast_to(pivot, (k, 2 * k)), 1, 0)
    work = work - ratio * pltpu.roll(work, 1, 0)
    pivot = pivot - ratio[:, :k] * beside
    return work[:, k:] * lax.rsqrt(pivot)


def near_identity(delta, strict, half):
    def lower(value):
        return jnp.where(strict, value, jnp.where(half, 0.5 * value, 0.0))

    def pair(value):
        one = value.astype(BF16)
        return one, (value - one.astype(F32)).astype(BF16)

    d1, d2 = pair(delta)
    right = jnp.concatenate([d1, d2, d1], axis=0)
    y = -lower(delta)
    for _ in range(2):
        y1, y2 = pair(y)
        outer = y + dot(jnp.concatenate([y1, y1, y2], axis=1), right)
        o1, o2 = pair(outer)
        square = dot_t(jnp.concatenate([o1, o1, o2], axis=1), jnp.concatenate([y1, y2, y1], axis=1))
        error = lower(delta + outer + outer.T + square)
        e1, e2 = pair(error)
        y = y - error - dot_of_stack([e1, e1, e2], [y1, y2, y1])
    return y


def factor_kernel(scale, gram_ref, high_ref, low_ref, upper_ref, y_ref):
    k = gram_ref.shape[0]
    pair = gram_ref[:, 0, :]
    high, low = pair[:, :k], pair[:, k:]
    row = lax.broadcasted_iota(jnp.int32, (k, k), 0)
    lane = lax.broadcasted_iota(jnp.int32, (k, k), 1)
    eye = row == lane
    diagonal = jnp.where(eye, high, 0.0)
    size_row, inverse_row = power_below(jnp.sum(diagonal, axis=0, keepdims=True), square=True)
    _, inverse_column = power_below(jnp.sum(diagonal, axis=1, keepdims=True), square=True)
    unit = inverse_column * inverse_row
    high = high * unit
    low = low * unit
    gram_digits = digits(high * 32.0, 6, extra=low * 32.0)
    guess = eliminate(high)
    top, top_inverse = power_below(jnp.max(jnp.abs(guess), axis=1, keepdims=True))
    guess_digits = digits(guess * top_inverse * 64.0, 3)
    exact = sum(d.astype(F32) * 256.0**-i for i, d in enumerate(guess_digits))
    exact = exact * (top * (1.0 / 64.0))
    guess_stack = jnp.concatenate(guess_digits, axis=0)
    counts = dot(guess_stack, jnp.concatenate(gram_digits, axis=1))
    high, low = levels_to_pair(level_sums(counts, k, 3, 6))
    product = (high + low) * (top * 2.0**-11)
    to_digits = top * 2.0**-6
    product_digits = digits(high * to_digits, 6, extra=low * to_digits)
    counts = dot_t(jnp.concatenate(product_digits, axis=0), guess_stack)
    high, low = levels_to_pair(level_sums(counts, k, 6, 3))
    top_row = jnp.sum(jnp.where(eye, top, 0.0), axis=0, keepdims=True)
    unit = 2.0**-11 * top_row
    high = high * unit
    low = low * unit
    delta = jnp.where(eye, high - 1.0, high) + low
    worst = jnp.max(jnp.abs(delta))
    small = worst < 2.0**-9

    @pl.when(small)
    def _():
        y_ref[...] = near_identity(delta, row > lane, eye)

    @pl.when(jnp.logical_not(small))
    def _():
        y_ref[...] = eliminate(high + low) - eye.astype(F32)

    y = y_ref[...]
    rest = dot_full(y, exact)
    high, low = two_sum(exact, rest)
    unit = inverse_row * scale
    high_ref[...] = high * unit
    low_ref[...] = low * unit
    upper = product + dot_full(y, product)
    upper_ref[...] = jnp.where(row <= lane, upper, 0.0) * (size_row * (1.0 / scale))


def factor(gram, scale):
    k = gram.shape[0]
    return pl.pallas_call(
        lambda *refs: factor_kernel(scale, *refs),
        out_shape=(in_vmem(k, k), in_vmem(k, k), jax.ShapeDtypeStruct((k, k), F32)),
        in_specs=[VMEM_SPEC],
        out_specs=(VMEM_SPEC, VMEM_SPEC, VMEM_SPEC),
        scratch_shapes=[pltpu.VMEM((k, k), F32)],
        compiler_params=SMALL,
        name="factor",
    )(vmem(gram))


def basis_kernel(w_ref, high_ref, low_ref, out_ref, result, sems):
    _, nx, _ = result.shape
    p1, p2, p3 = split3(high_ref[...])
    p4 = low_ref[...].astype(BF16)
    left = jnp.concatenate([p1, p1, p1, p2, p2, p3, p4], axis=1)
    copies = []
    for x in range(nx):
        w1, w2, w3 = split3(w_ref[x])
        right = jnp.concatenate([w3, w2, w1, w2, w1, w1, w1], axis=0)
        result[:, x, :] = dot(left, right)
        if (x + 1) % 8 == 0:
            rows = pl.ds(x - 7, 8)
            copies.append(pltpu.make_async_copy(result.at[:, rows, :], out_ref.at[:, rows, :], sems.at[x // 8]))
            copies[-1].start()
    for copy in copies:
        copy.wait()


def basis_of(w, high, low):
    nx, k, plane = w.shape
    return pl.pallas_call(
        basis_kernel,
        out_shape=jax.ShapeDtypeStruct((k, nx, plane), F32),
        in_specs=[VMEM_SPEC] * 3,
        out_specs=pl.BlockSpec(memory_space=pltpu.HBM),
        scratch_shapes=[pltpu.VMEM((k, nx, plane), F32), pltpu.SemaphoreType.DMA((nx // 8,))],
        compiler_params=SMALL,
        name="basis",
    )(vmem(w), vmem(high), vmem(low))


def device_program(vectors, reaction):
    _, nx, plane = vectors.shape
    peers = lax.axis_size(SFC_SUB)
    me = lax.axis_index(SFC_SUB)
    flags = jnp.stack([me % 2, (me > 0).astype(me.dtype), (me < peers - 1).astype(me.dtype)])
    inner, outer, vectors, reaction, table = borders(flags, vectors, reaction, jnp.asarray(tables()))
    across = [(i, i + 1) for i in range(1, peers - 1, 2)]
    within = [(i, i + 1) for i in range(0, peers, 2)]
    outer = lax.ppermute(outer, SFC_SUB, across + [(b, a) for a, b in across])
    inner = lax.ppermute(inner, SFC_SUB, within + [(b, a) for a, b in within])
    begun = begin(vectors, reaction, table)
    w, gram = operator_and_gram(flags, reaction, inner, outer, table, begun)
    gram = sum_over_devices(gram)
    high, low, upper = factor(gram, math.sqrt(peers * nx * plane))
    return basis_of(w, high, low), upper


def solution(mesh):
    torus = Mesh(mesh.devices.reshape(16, 8, 4, 2), ("sfc_0", "sfc_1", "sub_0", "sub_1"))
    in_specs = (P(None, SFC_SUB, None), P(SFC_SUB, None))
    out_specs = (P(None, SFC_SUB, None), P())
    return jax.shard_map(device_program, mesh=torus, in_specs=in_specs, out_specs=out_specs, check_vma=False)
```

```python
import math

import jax
import jax.numpy as jnp
import numpy as np
from jax import lax
from jax.experimental import pallas as pl
from jax.experimental.pallas import tpu as pltpu
from jax.sharding import Mesh
from jax.sharding import PartitionSpec as P

NY = 32
NL = 8
PLANE = NY * NL
POWERS = 3
SFC_SUB = ("sfc_0", "sfc_1", "sub_0", "sub_1")
FAR = ("sfc_0",)
NEAR = ("sfc_1", "sub_0", "sub_1")
DELTA_MASS = 0.5
F32 = jnp.float32
BF16 = jnp.bfloat16


SMALL = pltpu.CompilerParams(vmem_limit_bytes=24 * 2**20)
VMEM_SPEC = pl.BlockSpec(memory_space=pltpu.VMEM)


def in_vmem(*shape):
    return pltpu.VMEM(shape, F32)


def vmem(array):
    return pltpu.with_memory_space_constraint(array, pltpu.VMEM)


def hbm(array):
    return pltpu.with_memory_space_constraint(array, pltpu.HBM)


def line_tables(count):
    index = np.arange(count)
    offset = index[:, None] - index[None, :]
    near = (np.abs(offset) == 1).astype(np.float32)
    same = (offset == 0).astype(np.float32)
    return 4.0 * same + near, 2.0 * same - near


def tables():
    mass_across, stiff_across = line_tables(NY)
    mass_layers, stiff_layers = line_tables(NL)
    mass = np.kron(mass_layers, mass_across)
    stiff = (
        6.0 * (np.kron(mass_layers, stiff_across) + np.kron(stiff_layers, mass_across))
        + DELTA_MASS * mass
    )
    return np.concatenate([stiff - 6.0 * mass, 4.0 * stiff + 12.0 * mass], axis=1).astype(BF16)


def split3(value):
    one = value.astype(BF16)
    rest = value - one.astype(F32)
    two = rest.astype(BF16)
    three = (rest - two.astype(F32)).astype(BF16)
    return one, two, three


def dot(a, b):
    return lax.dot_general(a, b, (((1,), (0,)), ((), ())), preferred_element_type=F32)


def dot_t(a, b):
    return lax.dot_general(a, b, (((1,), (1,)), ((), ())), preferred_element_type=F32)


def two_sum(a, b):
    s = a + b
    t = s - a
    return s, (a - (s - t)) + (b - t)


def power_below(x, square=False):
    low = -60 if square else -120
    p = jnp.full_like(x, 2.0**low)
    q = jnp.full_like(x, 2.0**-low)
    for k in (64, 32, 16, 8, 4, 2, 1) if square else (128, 64, 32, 16, 8, 4, 2, 1):
        half = 2.0 ** (k // 2) if k > 1 else 2.0
        up = p * half * (half if k > 1 else 1.0)
        down = q * (1.0 / half) * (1.0 / half if k > 1 else 1.0)
        fits = (up * up if square else up) <= x
        p, q = jnp.where(fits, up, p), jnp.where(fits, down, q)
    return p, q


def digits(value, count, extra=None, extra_at=3):
    out = []
    rest = value
    for i in range(count):
        digit = jnp.round(rest)
        out.append(digit.astype(BF16))
        rest = rest - digit
        if extra is not None and i == extra_at - 1:
            rest = rest + extra * (256.0 ** (extra_at - 1))
        rest = rest * 256.0
    return out


def levels_to_pair(levels):
    high = levels[-1]
    low = jnp.zeros_like(high)
    for level in reversed(levels[:-1]):
        high, err = two_sum(level, high * (1.0 / 256.0))
        low = low * (1.0 / 256.0) + err
    return high, low


def border_kernel(odd_ref, vec_ref, react_ref, table_ref, inner_ref, outer_ref, own_ref, own_react_ref, own_table_ref, sems):
    k, nx, plane = vec_ref.shape
    parts = 4
    copies = []
    for part in range(parts):
        rows = pl.ds(part * (k // parts), k // parts)
        copies.append(pltpu.make_async_copy(vec_ref.at[rows], own_ref.at[rows], sems.at[part]))
    copies.append(pltpu.make_async_copy(react_ref, own_react_ref, sems.at[parts]))
    copies.append(pltpu.make_async_copy(table_ref, own_table_ref, sems.at[parts + 1]))
    for copy in copies:
        copy.start()
    copies[-2].wait()
    odd = odd_ref[0]

    def fill(ref, start, rows):
        for j in range(POWERS):
            ref[j, rows, :] = own_ref[rows, start + j, :]
            if rows.start == 0:
                ref[j, k:, :] = jnp.broadcast_to(own_react_ref[start + j : start + j + 1, :], (8, plane))

    for part in range(parts):
        rows = pl.ds(part * (k // parts), k // parts)
        copies[part].wait()

        @pl.when(odd == 0)
        def _():
            fill(inner_ref, nx - POWERS, rows)
            fill(outer_ref, 0, rows)

        @pl.when(odd != 0)
        def _():
            fill(inner_ref, 0, rows)
            fill(outer_ref, nx - POWERS, rows)

    copies[-1].wait()


def borders(odd, vectors, reaction, table):
    k, _, plane = vectors.shape
    shape = in_vmem(POWERS, k + 8, plane)
    anywhere = pl.BlockSpec(memory_space=pltpu.HBM)
    return pl.pallas_call(
        border_kernel,
        out_shape=(shape, shape, in_vmem(*vectors.shape), in_vmem(*reaction.shape), pltpu.VMEM(table.shape, table.dtype)),
        in_specs=[pl.BlockSpec(memory_space=pltpu.SMEM), anywhere, anywhere, anywhere],
        out_specs=(VMEM_SPEC,) * 5,
        scratch_shapes=[pltpu.SemaphoreType.DMA((6,))],
        compiler_params=SMALL,
        name="borders",
    )(odd, hbm(vectors), hbm(reaction), hbm(table))


def products(field, both, table, start, count):
    k = field.shape[1]
    n = count * k
    one, two, three = split3(field[pl.ds(start, count)].reshape(n, PLANE))
    parts = dot(jnp.concatenate([one, two, three], axis=0), table)
    both[pl.ds(start, count)] = (parts[:n] + parts[n : 2 * n] + parts[2 * n :]).reshape(count, k, 2 * PLANE)


def begin_kernel(vec_ref, react_ref, table_ref, own, own_both, first, first_both):
    _, nx, _ = vec_ref.shape
    for x in range(nx):
        own[x] = vec_ref[:, x, :]
    table = table_ref[...]

    def own_products(i, _):
        products(own, own_both, table, 0, nx)
        return 0

    lax.fori_loop(0, 1, own_products, 0)

    def inside(x, _):
        first[x - 1] = combination(own_both, own, react_ref, x, x)
        return 0

    lax.fori_loop(1, nx - 1, inside, 0, unroll=7)

    def first_products(i, _):
        products(first, first_both, table, 0, nx - 2)
        return 0

    lax.fori_loop(0, 1, first_products, 0)


def combination(both, field, react, x, at):
    return (both[x - 1, :, :PLANE] + both[x + 1, :, :PLANE] + both[x, :, PLANE:]) * (1.0 / 216.0) + react[
        pl.ds(at, 1), :
    ] * field[x]


def begin(vectors, reaction, table):
    k, nx, plane = vectors.shape
    return pl.pallas_call(
        begin_kernel,
        out_shape=(
            in_vmem(nx, k, plane),
            in_vmem(nx, k, 2 * plane),
            in_vmem(nx - 2, k, plane),
            in_vmem(nx - 2, k, 2 * plane),
        ),
        in_specs=[VMEM_SPEC] * 3,
        out_specs=(VMEM_SPEC,) * 4,
        cost_estimate=pl.CostEstimate(flops=12 * (nx + nx - 2) * k * plane * plane, bytes_accessed=0, transcendentals=0),
        compiler_params=SMALL,
        name="begin",
    )(vmem(vectors), vmem(reaction), vmem(table))


def operator_kernel(k, nx, flags_ref, react_ref, inner_ref, outer_ref, table_ref, own, own_both, first, first_both, w_ref, gram_ref, field, both, react):
    halo = POWERS
    total = nx + 2 * halo
    top = halo + nx
    odd = flags_ref[0]
    low_inside = flags_ref[1].astype(F32)
    high_inside = flags_ref[2].astype(F32)
    react[halo:top] = react_ref[...]

    def fill(low_ref, high_ref):
        field[0:halo] = low_ref[:, :k, :]
        field[top:total] = high_ref[:, :k, :]
        react[0:halo] = low_ref[:, k, :]
        react[top:total] = high_ref[:, k, :]

    @pl.when(odd == 0)
    def _():
        fill(outer_ref, inner_ref)

    @pl.when(odd != 0)
    def _():
        fill(inner_ref, outer_ref)

    table = table_ref[...]

    def keep(x):
        return jnp.where(x < halo, low_inside, jnp.where(x >= top, high_inside, 1.0))

    def step(x, _):
        field[x] = combination(both, field, react, x, x) * keep(x)
        return 0

    def ends(body, low, high, count):
        lax.fori_loop(0, 2 * count, lambda i, c: body(jnp.where(i < count, low + i, high + i - count), c), 0, unroll=count)

    def border_products(i, _):
        products(field, both, table, i * top, halo)
        return 0

    lax.fori_loop(0, 2, border_products, 0)

    def own_edge(x, _):
        field[x] = own[x - halo]
        both[x] = own_both[x - halo]
        return 0

    ends(own_edge, halo, top - 2, 2)
    ends(step, 1, top - 1, 3)

    def edge_products(i, _):
        products(field, both, table, 1 + i * (top - 2), halo)
        return 0

    lax.fori_loop(0, 2, edge_products, 0)

    def first_edge(x, _):
        field[x] = first[x - halo - 1]
        both[x] = first_both[x - halo - 1]
        return 0

    ends(first_edge, halo + 1, top - 3, 2)
    ends(step, 2, top - 2, 3)

    def inside(x, _):
        field[x] = combination(first_both, first, react, x - halo - 1, x)
        return 0

    lax.fori_loop(halo + 2, top - 2, inside, 0, unroll=6)

    def third_products(i, _):
        products(field, both, table, 2, total - 4)
        return 0

    lax.fori_loop(0, 1, third_products, 0)

    def last(x, _):
        w_ref[x - halo] = combination(both, field, react, x, x)
        return 0

    lax.fori_loop(halo, top, last, 0, unroll=8)
    peak = jnp.abs(w_ref[0])
    for x in range(1, nx):
        peak = jnp.maximum(peak, jnp.abs(w_ref[x]))
    peak = jnp.max(peak, axis=1, keepdims=True)
    size, inverse = power_below(peak)
    scale = inverse * 64.0
    slices = 4
    group = 4
    pairs = None
    for start in range(0, nx, group):
        parts = [[] for _ in range(slices)]
        for x in range(start, start + group):
            for s, digit in enumerate(digits(w_ref[x] * scale, slices)):
                parts[s].append(digit)
        stack = jnp.concatenate([jnp.concatenate(p, axis=1) for p in parts], axis=0)
        counts = dot_t(stack, stack)
        block = [[counts[i * k : (i + 1) * k, j * k : (j + 1) * k] for j in range(slices)] for i in range(slices)]
        tail = [
            sum(block[i][level - i] for i in range(slices) if 0 <= level - i < slices)
            for level in range(3, 2 * slices - 1)
        ]
        rest = tail[-1]
        for value in reversed(tail[:-1]):
            rest = value + rest * (1.0 / 256.0)
        terms = [
            rest * 2.0**-24,
            block[1][1] * 2.0**-16,
            (block[0][2] + block[2][0]) * 2.0**-16,
            block[0][1] * 2.0**-8,
            block[1][0] * 2.0**-8,
            block[0][0],
        ]
        for term in terms:
            if pairs is None:
                pairs = (term, jnp.zeros_like(term))
            else:
                high, err = two_sum(pairs[0], term)
                pairs = (high, pairs[1] + err)
    high, err = two_sum(pairs[0], pairs[1])
    row = size * (1.0 / 64.0)
    eye = lax.broadcasted_iota(jnp.int32, (k, k), 0) == lax.broadcasted_iota(jnp.int32, (k, k), 1)
    column = jnp.sum(jnp.where(eye, row, 0.0), axis=0, keepdims=True)
    gram_ref[:, 0, :] = jnp.concatenate([high * row * column, err * row * column], axis=1)


def operator_and_gram(flags, reaction, inner, outer, table, begun):
    nx, k, plane = begun[0].shape
    total = nx + 2 * POWERS
    smem = pl.BlockSpec(memory_space=pltpu.SMEM)
    return pl.pallas_call(
        lambda *refs: operator_kernel(k, nx, *refs),
        out_shape=(in_vmem(nx, k, plane), in_vmem(k, 1, 2 * k)),
        in_specs=[smem] + [VMEM_SPEC] * 8,
        out_specs=(VMEM_SPEC, VMEM_SPEC),
        scratch_shapes=[
            pltpu.VMEM((total, k, plane), F32),
            pltpu.VMEM((total, k, 2 * plane), F32),
            pltpu.VMEM((total + 18, plane), F32),
        ],
        cost_estimate=pl.CostEstimate(flops=2 * 3 * 30 * k * plane * 2 * plane, bytes_accessed=0, transcendentals=0),
        compiler_params=SMALL,
        name="operator_gram",
    )(flags, vmem(reaction), vmem(inner), vmem(outer), vmem(table), *map(vmem, begun))


def pair_sum_kernel(parts_ref, out_ref):
    value = parts_ref[:, 0, :]
    width = value.shape[1]
    half = width // 2
    error = jnp.zeros_like(value)
    while value.shape[0] > 1:
        n = value.shape[0] // 2
        value, err = two_sum(value[:n], value[n:])
        error = error[:n] + error[n:] + err
    low = pltpu.roll(value, half, 1) + error
    high, err = two_sum(value, low)
    lane = lax.broadcasted_iota(jnp.int32, value.shape, 1)
    row = jnp.where(lane < half, high, pltpu.roll(err, half, 1))
    out_ref[:, 0, :] = jnp.broadcast_to(row, (out_ref.shape[0], width))


def pair_sum(parts, copies):
    return pl.pallas_call(
        pair_sum_kernel,
        out_shape=in_vmem(copies, 1, parts.shape[2]),
        in_specs=[VMEM_SPEC],
        out_specs=VMEM_SPEC,
        compiler_params=SMALL,
        name="pair_sum",
    )(vmem(parts))


def sum_over_devices(gram):
    near = lax.axis_size(NEAR)
    far = lax.axis_size(FAR)
    rows = lax.all_to_all(gram, NEAR, 0, 0)
    mine = pair_sum(rows, far)
    mine = pair_sum(lax.all_to_all(mine, FAR, 0, 0), near)
    return lax.all_to_all(mine, NEAR, 0, 0)


def level_sums(counts, k, rows, columns):
    out = []
    for level in range(rows + columns - 1):
        terms = [
            counts[i * k : (i + 1) * k, (level - i) * k : (level - i + 1) * k]
            for i in range(rows)
            if 0 <= level - i < columns
        ]
        total = terms[0]
        for term in terms[1:]:
            total = total + term
        out.append(total)
    return out


def dot_of_stack(a_parts, b_parts):
    return dot(jnp.concatenate(a_parts, axis=1), jnp.concatenate(b_parts, axis=0))


def dot_full(a, b):
    a1, a2, a3 = split3(a)
    b1, b2, b3 = split3(b)
    return dot_of_stack([a1, a1, a2, a1, a2, a3], [b1, b2, b1, b3, b2, b1])


def eliminate(square):
    k = square.shape[0]
    row = lax.broadcasted_iota(jnp.int32, (k, k), 0)
    lane = lax.broadcasted_iota(jnp.int32, (k, k), 1)
    eye = (row == lane).astype(F32)
    block = 8
    work = jnp.concatenate([square, eye], axis=1)
    done = []
    for start in range(0, k, block):
        rows = work.shape[0]
        columns = [jnp.broadcast_to(work[:, start + a : start + a + 1], (rows, 2 * k)) for a in range(block)]
        below = lax.broadcasted_iota(jnp.int32, (rows, 2 * k), 0)
        for a in range(0, block, 2):
            one, two = columns[a], columns[a + 1]
            p, q, r = one[a : a + 1, :], two[a : a + 1, :], two[a + 1 : a + 2, :]
            inverse = 1.0 / (p * r - q * q)
            first = jnp.where(below > a + 1, (one * r - two * q) * inverse, 0.0)
            second = jnp.where(below > a + 1, (two * p - one * q) * inverse, 0.0)
            for b in range(a + 2, block):
                columns[b] = columns[b] - (first * columns[b][a : a + 1, :] + second * columns[b][a + 1 : a + 2, :])
            work = work - (first * work[a : a + 1, :] + second * work[a + 1 : a + 2, :])
        done.append(work[:block])
        work = work[block:]
    work = jnp.concatenate(done, axis=0)
    pivot = jnp.sum(work[:, :k] * eye, axis=1, keepdims=True)
    beside = jnp.sum(jnp.where((row == lane + 1) & (row % 2 == 1), work[:, :k], 0.0), axis=1, keepdims=True)
    ratio = beside / pltpu.roll(jnp.broadcast_to(pivot, (k, 2 * k)), 1, 0)
    work = work - ratio * pltpu.roll(work, 1, 0)
    pivot = pivot - ratio[:, :k] * beside
    return work[:, k:] * lax.rsqrt(pivot)


def near_identity(delta, strict, half):
    def lower(value):
        return jnp.where(strict, value, jnp.where(half, 0.5 * value, 0.0))

    def pair(value):
        one = value.astype(BF16)
        return one, (value - one.astype(F32)).astype(BF16)

    d1, d2 = pair(delta)
    right = jnp.concatenate([d1, d2, d1], axis=0)
    y = -lower(delta)
    for _ in range(2):
        y1, y2 = pair(y)
        outer = y + dot(jnp.concatenate([y1, y1, y2], axis=1), right)
        o1, o2 = pair(outer)
        square = dot_t(jnp.concatenate([o1, o1, o2], axis=1), jnp.concatenate([y1, y2, y1], axis=1))
        error = lower(delta + outer + outer.T + square)
        e1, e2 = pair(error)
        y = y - error - dot_of_stack([e1, e1, e2], [y1, y2, y1])
    return y


def factor_kernel(scale, gram_ref, high_ref, low_ref, upper_ref, y_ref):
    k = gram_ref.shape[0]
    pair = gram_ref[:, 0, :]
    high, low = pair[:, :k], pair[:, k:]
    row = lax.broadcasted_iota(jnp.int32, (k, k), 0)
    lane = lax.broadcasted_iota(jnp.int32, (k, k), 1)
    eye = row == lane
    diagonal = jnp.where(eye, high, 0.0)
    size_row, inverse_row = power_below(jnp.sum(diagonal, axis=0, keepdims=True), square=True)
    _, inverse_column = power_below(jnp.sum(diagonal, axis=1, keepdims=True), square=True)
    unit = inverse_column * inverse_row
    high = high * unit
    low = low * unit
    gram_digits = digits(high * 32.0, 6, extra=low * 32.0)
    guess = eliminate(high)
    top, top_inverse = power_below(jnp.max(jnp.abs(guess), axis=1, keepdims=True))
    guess_digits = digits(guess * top_inverse * 64.0, 3)
    exact = sum(d.astype(F32) * 256.0**-i for i, d in enumerate(guess_digits))
    exact = exact * (top * (1.0 / 64.0))
    guess_stack = jnp.concatenate(guess_digits, axis=0)
    counts = dot(guess_stack, jnp.concatenate(gram_digits, axis=1))
    high, low = levels_to_pair(level_sums(counts, k, 3, 6))
    product = (high + low) * (top * 2.0**-11)
    to_digits = top * 2.0**-6
    product_digits = digits(high * to_digits, 6, extra=low * to_digits)
    counts = dot_t(jnp.concatenate(product_digits, axis=0), guess_stack)
    high, low = levels_to_pair(level_sums(counts, k, 6, 3))
    top_row = jnp.sum(jnp.where(eye, top, 0.0), axis=0, keepdims=True)
    unit = 2.0**-11 * top_row
    high = high * unit
    low = low * unit
    delta = jnp.where(eye, high - 1.0, high) + low
    worst = jnp.max(jnp.abs(delta))
    small = worst < 2.0**-9

    @pl.when(small)
    def _():
        y_ref[...] = near_identity(delta, row > lane, eye)

    @pl.when(jnp.logical_not(small))
    def _():
        y_ref[...] = eliminate(high + low) - eye.astype(F32)

    y = y_ref[...]
    rest = dot_full(y, exact)
    high, low = two_sum(exact, rest)
    unit = inverse_row * scale
    high_ref[...] = high * unit
    low_ref[...] = low * unit
    upper = product + dot_full(y, product)
    upper_ref[...] = jnp.where(row <= lane, upper, 0.0) * (size_row * (1.0 / scale))


def factor(gram, scale):
    k = gram.shape[0]
    return pl.pallas_call(
        lambda *refs: factor_kernel(scale, *refs),
        out_shape=(in_vmem(k, k), in_vmem(k, k), jax.ShapeDtypeStruct((k, k), F32)),
        in_specs=[VMEM_SPEC],
        out_specs=(VMEM_SPEC, VMEM_SPEC, VMEM_SPEC),
        scratch_shapes=[pltpu.VMEM((k, k), F32)],
        compiler_params=SMALL,
        name="factor",
    )(vmem(gram))


def basis_kernel(w_ref, high_ref, low_ref, out_ref, result, sems):
    k, nx, _ = result.shape
    p1, p2, p3 = split3(high_ref[...])
    p4 = low_ref[...].astype(BF16)
    left = jnp.concatenate(
        [
            jnp.concatenate([p1, p1, p1, p2], axis=1),
            jnp.concatenate([jnp.zeros_like(p1), p2, p4, p3], axis=1),
        ],
        axis=0,
    )
    copies = []
    for x in range(nx):
        w1, w2, w3 = split3(w_ref[x])
        both = dot(left, jnp.concatenate([w3, w2, w1, w1], axis=0))
        result[:, x, :] = both[:k] + both[k:]
        if (x + 1) % 8 == 0:
            rows = pl.ds(x - 7, 8)
            copies.append(pltpu.make_async_copy(result.at[:, rows, :], out_ref.at[:, rows, :], sems.at[x // 8]))
            copies[-1].start()
    for copy in copies:
        copy.wait()


def basis_of(w, high, low):
    nx, k, plane = w.shape
    return pl.pallas_call(
        basis_kernel,
        out_shape=jax.ShapeDtypeStruct((k, nx, plane), F32),
        in_specs=[VMEM_SPEC] * 3,
        out_specs=pl.BlockSpec(memory_space=pltpu.HBM),
        scratch_shapes=[pltpu.VMEM((k, nx, plane), F32), pltpu.SemaphoreType.DMA((nx // 8,))],
        compiler_params=SMALL,
        name="basis",
    )(vmem(w), vmem(high), vmem(low))


def device_program(vectors, reaction):
    _, nx, plane = vectors.shape
    peers = lax.axis_size(SFC_SUB)
    me = lax.axis_index(SFC_SUB)
    flags = jnp.stack([me % 2, (me > 0).astype(me.dtype), (me < peers - 1).astype(me.dtype)])
    inner, outer, vectors, reaction, table = borders(flags, vectors, reaction, jnp.asarray(tables()))
    across = [(i, i + 1) for i in range(1, peers - 1, 2)]
    within = [(i, i + 1) for i in range(0, peers, 2)]
    outer = lax.ppermute(outer, SFC_SUB, across + [(b, a) for a, b in across])
    inner = lax.ppermute(inner, SFC_SUB, within + [(b, a) for a, b in within])
    begun = begin(vectors, reaction, table)
    w, gram = operator_and_gram(flags, reaction, inner, outer, table, begun)
    gram = sum_over_devices(gram)
    high, low, upper = factor(gram, math.sqrt(peers * nx * plane))
    return basis_of(w, high, low), upper


def solution(mesh):
    torus = Mesh(mesh.devices.reshape(16, 8, 4, 2), ("sfc_0", "sfc_1", "sub_0", "sub_1"))
    in_specs = (P(None, SFC_SUB, None), P(SFC_SUB, None))
    out_specs = (P(None, SFC_SUB, None), P())
    return jax.shard_map(device_program, mesh=torus, in_specs=in_specs, out_specs=out_specs, check_vma=False)
```
